32 devices in a mesh: grp: 8 (over z, y), mem: 4 (over x, core).
Axes of the slice: x: 2, y: 2, z: 4, core: 2. Of those that a mesh axis runs over, the one named last changes fastest.
Arguments:
- queries: bfloat16 [8192, 2048], P(('grp', 'mem')), may hold values from -6 to 6
- keys: bfloat16 [8192, 2048], P(('grp', 'mem')), may hold values from -6 to 6
- values: bfloat16 [8192, 2048], P(('grp', 'mem')), may hold values from -6 to 6
- grad_out: bfloat16 [8192, 2048], P(('grp', 'mem')), may hold values from -0.125 to 0.125
- log_decay: float32 [8, 8192], P(None, ('grp', 'mem')), may hold values from -1.6 to 0
Outputs:
- grad_queries: bfloat16 [8192, 2048], P(('grp', 'mem'))
- grad_keys: bfloat16 [8192, 2048], P(('grp', 'mem'))
- grad_values: bfloat16 [8192, 2048], P(('grp', 'mem'))
The draws below stay inside these ranges and needn't reach their ends.
All inputs are finite; a program needn't handle non-finite values.
Results may differ from the reference program's by a relative error of at most 0.0052.
Values sent between devices are 32-bit elements; how exact they have to be, the bound alone decides.
A program may use at most 128 MiB of HBM per device.

```python
import jax
import jax.numpy as jnp
from jax import lax

HEAD_COUNT = 8
DK = 256
DV = 256
BLOCK = 128
TOK_DEV = 256
SEQUENCE_TOKENS = 8192


def draw_log_decay(key, part):
    base_key = jax.random.fold_in(key, 7)
    key_collection = jax.random.split(base_key, 6)
    order = jax.random.permutation(key_collection[0], HEAD_COUNT)
    fast_count = HEAD_COUNT // 2
    fast = order < fast_count
    fast_rate = jnp.exp(jax.random.uniform(key_collection[1], (HEAD_COUNT,), jnp.float32, jnp.log(1.0 / 50.0), jnp.log(1.0 / 30.0)))
    slow_rate = 0.3 / SEQUENCE_TOKENS
    decay_rates = jnp.where(fast, fast_rate, slow_rate)
    approximate = jnp.exp(jax.random.uniform(key_collection[2], (HEAD_COUNT, SEQUENCE_TOKENS), jnp.float32, jnp.log(0.5), jnp.log(2.0)))
    device_count = SEQUENCE_TOKENS // TOK_DEV
    device_factor = jnp.exp(jax.random.uniform(key_collection[3], (HEAD_COUNT, device_count), jnp.float32, jnp.log(0.5), jnp.log(2.0)))
    device_complete = jnp.repeat(device_factor, TOK_DEV, axis=1)
    spike_start = jax.random.randint(key_collection[4], (HEAD_COUNT, 2), 0, SEQUENCE_TOKENS)
    spike_length = jax.random.uniform(key_collection[5], (HEAD_COUNT, 2), jnp.float32, 0.22, 0.69)
    token_positions = jnp.arange(SEQUENCE_TOKENS)
    match_count = (token_positions[None, None, :] == spike_start[:, :, None]).astype(jnp.float32)
    spike_run = jnp.sum(match_count * spike_length[:, :, None], axis=1)
    return (-(decay_rates[:, None] * approximate * device_complete) - spike_run).astype(jnp.float32)


def block_levels(key, shape, cuts, least, high):
    level = 1.0
    for axis_at, parts in cuts:
        steps = jax.random.uniform(jax.random.fold_in(jax.random.fold_in(key, 6), axis_at), (parts,), jnp.float32, least / len(cuts), high / len(cuts))
        level = level * jnp.repeat(jnp.exp(steps), shape[axis_at] // parts).reshape((-1,) + (1,) * (len(shape) - 1 - axis_at))
    return level


def gaussian(stream_key, extent, scale, limit, pieces=(), kind=jnp.bfloat16):
    gain = block_levels(stream_key, extent, pieces, -0.22, 0.18) if pieces else 1.0
    values = jax.random.normal(stream_key, extent, jnp.float32) * scale * gain
    return jnp.minimum(jnp.maximum(values, -limit), limit).astype(kind)


def setup_inputs(seed: int = 0) -> dict:
    splits = jax.random.split(jax.random.key(seed), 6)
    queries = gaussian(splits[0], (SEQUENCE_TOKENS, HEAD_COUNT * DK), 1.0, 6.0, ((0, 32),))
    keys = gaussian(splits[1], (SEQUENCE_TOKENS, HEAD_COUNT * DK), 1.0, 6.0, ((0, 32),))
    values = gaussian(splits[2], (SEQUENCE_TOKENS, HEAD_COUNT * DV), 1.0, 6.0, ((0, 32),))
    grad_out = gaussian(splits[3], (SEQUENCE_TOKENS, HEAD_COUNT * DV), (2 * SEQUENCE_TOKENS ** -0.5), 0.125, ((0, 32),))
    log_decay = draw_log_decay(jax.random.fold_in(splits[5], 71), 0)
    return dict(queries=queries, keys=keys, values=values, grad_out=grad_out, log_decay=log_decay)


def block_factors(logs):
    cumul = jnp.cumsum(logs, axis=-1)
    ends = cumul[:, -1]
    width = logs.shape[-1]
    lower = jnp.tril(jnp.ones((width, width), dtype=bool))
    spread = cumul[:, :, None] - cumul[:, None, :]
    decay = jnp.where(lower, jnp.exp(jnp.where(lower, spread, 0.0)), 0.0)
    return cumul, ends, decay


def reference(queries, keys, values, grad_out, log_decay):
    count = SEQUENCE_TOKENS // BLOCK
    scale = DK ** -0.5
    query_blocks = queries.reshape(count, BLOCK, HEAD_COUNT, DK)
    key_blocks = keys.reshape(count, BLOCK, HEAD_COUNT, DK)
    value_blocks = values.reshape(count, BLOCK, HEAD_COUNT, DV)
    grad_blocks = grad_out.reshape(count, BLOCK, HEAD_COUNT, DV)
    log_blocks = jnp.transpose(log_decay.reshape(HEAD_COUNT, count, BLOCK), (1, 0, 2))

    def forward_step(state, inputs):
        query_now, key_now, value_now, grad_now, logs = inputs
        query32 = query_now.astype(jnp.float32)
        key32 = key_now.astype(jnp.float32)
        value32 = value_now.astype(jnp.float32)
        grad32 = grad_now.astype(jnp.float32)
        cumul, ends, decay = block_factors(logs)
        scores = jnp.einsum('the,she->hts', grad32, value32)
        weight_grad = lax.optimization_barrier((scores * decay).astype(jnp.bfloat16))
        inner = jnp.einsum('hts,shd->thd', weight_grad.astype(jnp.float32), key32)
        state_low = lax.optimization_barrier(state.astype(jnp.bfloat16))
        outer = jnp.einsum('the,hde->thd', grad32, state_low.astype(jnp.float32))
        outer = outer * jnp.exp(cumul).T[:, :, None]
        result = (scale * (inner + outer)).astype(jnp.bfloat16)
        tail = jnp.exp(ends[:, None] - cumul).T[:, :, None]
        keys_decayed = lax.optimization_barrier((key32 * tail).astype(jnp.bfloat16))
        update = jnp.einsum('shd,she->hde', keys_decayed.astype(jnp.float32), value32)
        state_next = jnp.exp(ends)[:, None, None] * state + update
        return state_next, result

    def reverse_step(state, inputs):
        query_now, key_now, value_now, grad_now, logs = inputs
        query32 = query_now.astype(jnp.float32)
        key32 = key_now.astype(jnp.float32)
        value32 = value_now.astype(jnp.float32)
        grad32 = grad_now.astype(jnp.float32)
        cumul, ends, decay = block_factors(logs)
        scores = jnp.einsum('the,she->hts', grad32, value32)
        weight_grad = lax.optimization_barrier((scores * decay).astype(jnp.bfloat16))
        attend = jnp.einsum('thd,shd->hts', query32, key32)
        weight_value = lax.optimization_barrier((attend * decay).astype(jnp.bfloat16))
        state_low = lax.optimization_barrier(state.astype(jnp.bfloat16)).astype(jnp.float32)
        tail = jnp.exp(ends[:, None] - cumul).T[:, :, None]
        key_grad = jnp.einsum('hts,thd->shd', weight_grad.astype(jnp.float32), query32)
        key_grad = key_grad + tail * jnp.einsum('she,hde->shd', value32, state_low)
        value_grad = jnp.einsum('hts,the->she', weight_value.astype(jnp.float32), grad32)
        value_grad = value_grad + tail * jnp.einsum('shd,hde->she', key32, state_low)
        queries_decayed = lax.optimization_barrier((query32 * jnp.exp(cumul).T[:, :, None]).astype(jnp.bfloat16))
        update = jnp.einsum('thd,the->hde', queries_decayed.astype(jnp.float32), grad32)
        state_next = jnp.exp(ends)[:, None, None] * state + update
        return state_next, ((scale * key_grad).astype(jnp.bfloat16), (scale * value_grad).astype(jnp.bfloat16))

    inputs = (query_blocks, key_blocks, value_blocks, grad_blocks, log_blocks)
    empty = jnp.zeros((HEAD_COUNT, DK, DV), jnp.float32)
    unused, grad_q = lax.scan(forward_step, empty, inputs)
    unused_too, pair = lax.scan(reverse_step, empty, inputs, reverse=True)
    grad_k, grad_v = pair
    return (grad_q.reshape(SEQUENCE_TOKENS, HEAD_COUNT * DK), grad_k.reshape(SEQUENCE_TOKENS, HEAD_COUNT * DK), grad_v.reshape(SEQUENCE_TOKENS, HEAD_COUNT * DV))
```

```python
import functools

import jax
import jax.numpy as jnp
from jax import lax
from jax.experimental import pallas as pl
from jax.experimental.pallas import tpu as pltpu
from jax.sharding import PartitionSpec as P

HEAD_COUNT = 8
DK = 256
DV = 256
BLOCK = 128
CORES = 2
KEYS, VALUES, QUERIES, GRADS = range(4)
MESH = pl.DeviceIdType.MESH
F32 = jnp.float32
BF16 = jnp.bfloat16


def dot(a, b, ca, cb):
    return lax.dot_general(a, b, (((ca,), (cb,)), ((), ())), preferred_element_type=F32)


def spread_rows(row):
    flat = jnp.broadcast_to(row, (BLOCK, BLOCK))
    return flat, flat.T


def wide(mat, width):
    return jnp.concatenate([mat] * (width // BLOCK), axis=1)


def retention_kernel(
    nx, ny, nz, logs_hbm, q_hbm, k_hbm, v_hbm, g_hbm, gq_ref, gk_ref, gv_ref,
    logs_ref, toks, cum, local, inner, total_buf, from_buf, peer_buf, back_buf,
    chip_buf, x_in, row_tot, y_in, plane_tot, z_in, acc, y_out, row_carry, x_out, carry,
    d_core, d_mate, d_x, d_y, d_z,
    s_logs, s_in, s_core, r_core, s_x, r_x, s_y, r_y, s_z, r_z,
    s_yout, r_yout, s_xout, r_xout, s_back, r_back, s_d, r_d,
):
    count = logs_ref.shape[1] // BLOCK
    scale = DK ** (-0.5)
    half = HEAD_COUNT // CORES
    wx = DK // nx
    wy = wx // ny
    chunks = [(d, k) for k in range(half) for d in range(2)]
    grp, mem = lax.axis_index("grp"), lax.axis_index("mem")
    z, y = grp // ny, lax.rem(grp, ny)
    x, core = mem // CORES, lax.rem(mem, CORES)
    mate = (grp, x * CORES + 1 - core)

    def x_id(to):
        return (grp, to * CORES + core)

    def y_id(to):
        return (z * ny + to, mem)

    def z_id(to):
        return (to * ny + y, mem)

    xs = [lax.rem(x + off, nx) for off in range(1, nx)]
    ys = [lax.rem(y + off, ny) for off in range(1, ny)]
    zs = [lax.rem(z + off, nz) for off in range(1, nz)]
    peers = [mate] + [x_id(o) for o in xs] + [y_id(o) for o in ys] + [z_id(o) for o in zs]
    barrier = pltpu.get_barrier_semaphore()
    for peer in peers:
        pl.semaphore_signal(barrier, inc=1, device_id=peer, device_id_type=MESH)

    def copy(src, dst, send, recv, device):
        return pltpu.make_async_remote_copy(
            src_ref=src, dst_ref=dst, send_sem=send, recv_sem=recv,
            device_id=device, device_id_type=MESH,
        )

    def go(*args):
        copy(*args).start()

    def landed(ref, sem):
        copy(ref, ref, s_back, sem, mate).wait_recv()

    def left(ref, sem):
        copy(ref, ref, sem, r_back.at[0], mate).wait_send()

    def members(d, size):
        return range(size) if d == 0 else range(size - 1, -1, -1)

    mine, theirs = core * half, (1 - core) * half

    def rows_of(c, size):
        return pl.ds(pl.multiple_of(c * size, size), size)

    def cols_of(head, size):
        return pl.ds(pl.multiple_of(head * size, size), size)

    def tokens_of(b):
        return pl.ds(b * BLOCK, BLOCK)

    load_logs = pltpu.make_async_copy(logs_hbm, logs_ref, s_logs)
    load_logs.start()
    for k in range(half):
        for head in (theirs + k, mine + k):
            part = cols_of(head, DK)
            for i, far in enumerate((k_hbm, v_hbm, q_hbm, g_hbm)):
                pltpu.make_async_copy(
                    far.at[:, part], toks.at[i, :, part], s_in.at[i // 2, head]
                ).start()

    def ready(pair, head):
        held = toks.at[pl.ds(2 * pair, 2), :, cols_of(head, DK)]
        pltpu.make_async_copy(held, held, s_in.at[pair, head]).wait()

    def tok(i, head, b):
        return toks[i, tokens_of(b), cols_of(head, DK)]

    load_logs.wait()
    carried = None
    for b in range(count):
        row = logs_ref[:, b * BLOCK:(b + 1) * BLOCK]
        lane = lax.broadcasted_iota(jnp.int32, row.shape, 1)
        step = 1
        while step < BLOCK:
            row = row + jnp.where(lane >= step, pltpu.roll(row, step, 1), 0.0)
            step *= 2
        whole = jnp.exp(row[:, BLOCK - 1:BLOCK])
        carried = whole if carried is None else carried * whole
        for h in range(HEAD_COUNT):
            cum[b, h] = row[h:h + 1, :]
    carried = jnp.broadcast_to(carried, (HEAD_COUNT, DV))
    for h in range(HEAD_COUNT):
        d_core[h] = carried[h:h + 1, :]

    def factors(head, b):
        row = cum[b, head]
        flat, cols = spread_rows(row)
        end = row[:, BLOCK - 1:BLOCK]
        return flat, cols, end

    def forward_total(head):
        ready(0, head)
        forward = None
        for b in range(count):
            _, cols, end = factors(head, b)
            kd = tok(KEYS, head, b).astype(F32) * wide(jnp.exp(end - cols), DK)
            whole = jnp.broadcast_to(jnp.exp(end), (1, DV))
            part = dot(kd.astype(BF16), tok(VALUES, head, b), 0, 0)
            if b > 0:
                local[0, b - 1, head] = forward
            forward = part if forward is None else whole * forward + part
        total_buf[0, head] = forward

    def reverse_total(head):
        ready(1, head)
        back = None
        for b in reversed(range(count)):
            _, cols, end = factors(head, b)
            qd = tok(QUERIES, head, b).astype(F32) * wide(jnp.exp(cols), DK)
            whole = jnp.broadcast_to(jnp.exp(end), (1, DV))
            part = dot(qd.astype(BF16), tok(GRADS, head, b), 0, 0)
            if b < count - 1:
                local[1, b, head] = back
            back = part if back is None else whole * back + part
        total_buf[1, head] = back

    lower = lax.broadcasted_iota(jnp.int32, (BLOCK, BLOCK), 0) >= lax.broadcasted_iota(
        jnp.int32, (BLOCK, BLOCK), 1
    )

    def intra(head):
        for b in range(count):
            flat, cols, _ = factors(head, b)
            decay = jnp.where(lower, jnp.exp(jnp.where(lower, cols - flat, 0.0)), 0.0)
            q, k = tok(QUERIES, head, b), tok(KEYS, head, b)
            v, g = tok(VALUES, head, b), tok(GRADS, head, b)
            wg = (dot(g, v, 1, 1) * decay).astype(BF16)
            wv = (dot(q, k, 1, 1) * decay).astype(BF16)
            inner[0, head, tokens_of(b), :] = dot(wg, k, 1, 0)
            inner[1, head, tokens_of(b), :] = dot(wg, q, 0, 0)
            inner[2, head, tokens_of(b), :] = dot(wv, g, 0, 0)

    def outer(d, head):
        coming = from_buf[d, head]
        weight = None
        for step, b in enumerate(members(d, count)):
            _, cols, end = factors(head, b)
            if step == 0:
                low = coming.astype(BF16)
            else:
                low = (local[d, b - 1 if d == 0 else b, head] + weight * coming).astype(BF16)
            whole = jnp.broadcast_to(jnp.exp(end), (1, DV))
            weight = whole if weight is None else weight * whole
            if d == 0:
                far = wide(jnp.exp(cols), DK) * dot(tok(GRADS, head, b), low, 1, 1)
                near = inner[0, head, tokens_of(b), :]
                gq_ref[tokens_of(b), cols_of(head, DK)] = (scale * (near + far)).astype(BF16)
            else:
                tail = wide(jnp.exp(end - cols), DK)
                near = inner[1, head, tokens_of(b), :]
                far = tail * dot(tok(VALUES, head, b), low, 1, 1)
                gk_ref[tokens_of(b), cols_of(head, DK)] = (scale * (near + far)).astype(BF16)
                near = inner[2, head, tokens_of(b), :]
                far = tail * dot(tok(KEYS, head, b), low, 1, 0)
                gv_ref[tokens_of(b), cols_of(head, DV)] = (scale * (near + far)).astype(BF16)

    first = core == 0

    def send_core(n, d, j):
        go(total_buf.at[d, theirs + j], peer_buf.at[d, j], s_core, r_core.at[n], mate)

    def join_cores(n, d, j):
        landed(peer_buf.at[d, j], r_core.at[n])
        own_d, peer_d = d_core[mine + j], d_mate[mine + j]
        one = jnp.ones_like(own_d)
        if d == 0:
            w_own, w_peer = jnp.where(first, peer_d, one), jnp.where(first, one, own_d)
        else:
            w_own, w_peer = jnp.where(first, one, peer_d), jnp.where(first, own_d, one)
        chip_buf[d, j] = w_own * total_buf[d, mine + j] + w_peer * peer_buf[d, j]
        for o in xs:
            go(chip_buf.at[d, j, rows_of(o, wx), :], x_in.at[x, d, j], s_x, r_x.at[n], x_id(o))
        x_in[x, d, j] = chip_buf[d, j, rows_of(x, wx), :]

    def fold(d, j, parts, decays, size):
        running = None
        for c in members(d, size):
            part = parts[c, d, j]
            running = part if running is None else decays[c, mine + j] * running + part
        return running

    def up_x(n, d, j):
        if n == 0:
            landed(d_x.at[pl.ds(0, nx - 1)], r_d.at[1])
            product = d_x[0]
            for c in range(1, nx):
                product = product * d_x[c]
            d_y[y] = product
            for o in ys:
                go(d_y.at[y], d_y.at[y], s_d.at[2], r_d.at[2], y_id(o))
        landed(x_in.at[pl.ds(0, nx - 1), d, j], r_x.at[n])
        row_tot[d, j] = fold(d, j, x_in, d_x, nx)
        for o in ys:
            go(row_tot.at[d, j, rows_of(o, wy), :], y_in.at[y, d, j], s_y, r_y.at[n], y_id(o))
        y_in[y, d, j] = row_tot[d, j, rows_of(y, wy), :]

    def up_y(n, d, j):
        if n == 0:
            if ny > 1:
                landed(d_y.at[pl.ds(0, ny - 1)], r_d.at[2])
            product = d_y[0]
            for c in range(1, ny):
                product = product * d_y[c]
            d_z[z] = product
            for t in zs:
                go(d_z.at[z], d_z.at[z], s_d.at[3], r_d.at[3], z_id(t))
        if ny > 1:
            landed(y_in.at[pl.ds(0, ny - 1), d, j], r_y.at[n])
        plane_tot[d, j] = fold(d, j, y_in, d_y, ny)
        for t in zs:
            c = copy(plane_tot.at[d, j], z_in.at[z, d, j], s_z, r_z.at[z, n], z_id(t))
            pl.when((t > z) if d == 0 else (t < z))(c.start)

    def spread(d, j, held, parts, decays, size, out):
        last = members(d, size)[-1]
        for c in members(d, size):
            out[c, d, j] = held
            if c != last:
                held = decays[c, mine + j] * held + parts[c, d, j]

    def over_z(n, d, j):
        if n == 0 and nz > 1:
            landed(d_z.at[pl.ds(0, nz - 1)], r_d.at[3])
        acc[...] = jnp.zeros((wy, DV), F32)
        for t in members(d, nz):
            @pl.when((t < z) if d == 0 else (t > z))
            def _():
                landed(z_in.at[t, d, j], r_z.at[t, n])
                acc[...] = d_z[t, mine + j] * acc[...] + z_in[t, d, j]
        spread(d, j, acc[...], y_in, d_y, ny, y_out)

    def send_y(n, d, j):
        for o in ys:
            go(y_out.at[o, d, j], row_carry.at[d, j, rows_of(y, wy), :], s_yout, r_yout.at[n], y_id(o))
        row_carry[d, j, rows_of(y, wy), :] = y_out[y, d, j]

    def down_y(n, d, j):
        if ny > 1:
            landed(row_carry.at[d, j, pl.ds(0, (ny - 1) * wy), :], r_yout.at[n])
        spread(d, j, row_carry[d, j], x_in, d_x, nx, x_out)
        for o in xs:
            go(x_out.at[o, d, j], carry.at[d, j, rows_of(x, wx), :], s_xout, r_xout.at[n], x_id(o))
        carry[d, j, rows_of(x, wx), :] = x_out[x, d, j]

    def down_x(n, d, j):
        landed(carry.at[d, j, pl.ds(0, (nx - 1) * wx), :], r_xout.at[n])
        near = first if d == 0 else jnp.logical_not(first)

        @pl.when(near)
        def _():
            got = carry[d, j]
            back_buf[d, j] = d_core[mine + j] * got + total_buf[d, mine + j]
            from_buf[d, mine + j] = got

        @pl.when(jnp.logical_not(near))
        def _():
            got = carry[d, j]
            back_buf[d, j] = got
            from_buf[d, mine + j] = d_mate[mine + j] * got + peer_buf[d, j]

        go(back_buf.at[d, j], from_buf.at[d, mine + j], s_back, r_back.at[n], mate)
        outer(d, mine + j)

    def finish(n, d, j):
        landed(from_buf.at[d, theirs + j], r_back.at[n])
        outer(d, theirs + j)

    todo = []
    for k in range(half):
        todo += [
            (forward_total, theirs + k, 2 * k), (reverse_total, theirs + k, 2 * k + 1),
            (forward_total, mine + k, None), (reverse_total, mine + k, None),
        ]
    after = {}
    for n in range(len(chunks)):
        after[min(4 * (n // 2) + 4 + n % 2, len(todo) - 1 + n % 2)] = n
    for i, (work, head, n) in enumerate(todo):
        work(head)
        if i == 0:
            pl.semaphore_wait(barrier, len(peers))
            go(d_core, d_mate, s_d.at[0], r_d.at[0], mate)
        if n is not None:
            send_core(n, *chunks[n])
        if i in after:
            m = after[i]
            if m == 0:
                landed(d_mate, r_d.at[0])
                d_x[x] = d_core[...] * d_mate[...]
                for o in xs:
                    go(d_x.at[x], d_x.at[x], s_d.at[1], r_d.at[1], x_id(o))
            join_cores(m, *chunks[m])
    for i in sorted(after):
        if i >= len(todo):
            join_cores(after[i], *chunks[after[i]])

    stages = ((0, up_x), (1, up_y), (3, over_z), (3, send_y), (4, down_y))
    for slot in range(len(chunks) + 4):
        for lag, stage in stages:
            n = slot - lag
            if 0 <= n < len(chunks):
                stage(n, *chunks[n])
            if lag == 0:
                for h in range(slot, HEAD_COUNT, len(chunks)) if slot < len(chunks) else ():
                    intra(h)
    for n, (d, j) in enumerate(chunks):
        down_x(n, d, j)
        if n > 0:
            finish(n - 1, *chunks[n - 1])
    finish(len(chunks) - 1, *chunks[-1])

    left(peer_buf, s_core)
    left(x_in.at[pl.ds(0, nx - 1)], s_x)
    left(x_out.at[pl.ds(0, nx - 1)], s_xout)
    left(back_buf, s_back)
    left(d_mate, s_d.at[0])
    left(d_x.at[pl.ds(0, nx - 1)], s_d.at[1])
    if ny > 1:
        left(y_in.at[pl.ds(0, ny - 1)], s_y)
        left(y_out.at[pl.ds(0, ny - 1)], s_yout)
        left(d_y.at[pl.ds(0, ny - 1)], s_d.at[2])
    if nz > 1:
        left(z_in.at[pl.ds(0, nz - 1), 0], s_z)
        left(d_z.at[pl.ds(0, nz - 1)], s_d.at[3])


def write_kernel(gq_ref, gk_ref, gv_ref, gq_hbm, gk_hbm, gv_hbm, sems):
    copies = [
        pltpu.make_async_copy(near, far, sems.at[i])
        for i, (near, far) in enumerate(((gq_ref, gq_hbm), (gk_ref, gk_hbm), (gv_ref, gv_hbm)))
    ]
    for c in copies:
        c.start()
    for c in copies:
        c.wait()


def body(nx, ny, nz, queries, keys, values, grad_out, log_decay):
    tokens = queries.shape[0]
    count = tokens // BLOCK
    half = HEAD_COUNT // CORES
    wx = DK // nx
    wy = wx // ny
    n = 2 * half
    vm = pl.BlockSpec(memory_space=pltpu.VMEM)
    hbm = pl.BlockSpec(memory_space=pltpu.HBM)
    dma = pltpu.SemaphoreType.DMA

    def states(*lead):
        return pltpu.VMEM(lead + (DV,), F32)

    def decays(*lead):
        return pltpu.VMEM(lead + (HEAD_COUNT, 1, DV), F32)

    out = jax.ShapeDtypeStruct((tokens, HEAD_COUNT * DK), BF16)
    grads = pl.pallas_call(
        functools.partial(retention_kernel, nx, ny, nz),
        out_shape=(out, out, out),
        in_specs=[hbm] * 5,
        out_specs=(vm, vm, vm),
        scratch_shapes=[
            pltpu.VMEM((HEAD_COUNT, tokens), F32),
            pltpu.VMEM((4, tokens, HEAD_COUNT * DK), BF16),
            pltpu.VMEM((count, HEAD_COUNT, 1, BLOCK), F32),
            states(2, max(1, count - 1), HEAD_COUNT, DK),
            states(3, HEAD_COUNT, tokens),
            states(2, HEAD_COUNT, DK), states(2, HEAD_COUNT, DK),
            states(2, half, DK), states(2, half, DK),
            states(2, half, DK), states(nx, 2, half, wx), states(2, half, wx),
            states(ny, 2, half, wy), states(2, half, wy), states(nz, 2, half, wy), states(wy),
            states(ny, 2, half, wy), states(2, half, wx),
            states(nx, 2, half, wx), states(2, half, DK),
            decays(), decays(), decays(nx), decays(ny), decays(nz),
            dma, dma((2, HEAD_COUNT)),
            dma, dma((n,)), dma, dma((n,)), dma, dma((n,)), dma, dma((nz, n)),
            dma, dma((n,)), dma, dma((n,)), dma, dma((n,)), dma((4,)), dma((4,)),
        ],
        compiler_params=pltpu.CompilerParams(collective_id=0, has_side_effects=True, vmem_limit_bytes=52 << 20),
        name="retention",
    )(log_decay, queries, keys, values, grad_out)
    return pl.pallas_call(
        write_kernel,
        out_shape=(out, out, out),
        in_specs=[vm] * 3,
        out_specs=(hbm, hbm, hbm),
        scratch_shapes=[dma((3,))],
        name="write",
    )(*grads)


def solution(mesh):
    nx = mesh.shape["mem"] // CORES
    ny = nx if mesh.shape["grp"] % nx == 0 else 1
    nz = mesh.shape["grp"] // ny
    tokens = P(("grp", "mem"), None)
    return jax.shard_map(
        functools.partial(body, nx, ny, nz),
        mesh=mesh,
        in_specs=(tokens, tokens, tokens, tokens, P(None, ("grp", "mem"))),
        out_specs=(tokens, tokens, tokens),
        check_vma=False,
    )
```

```python
import functools

import jax
import jax.numpy as jnp
from jax import lax
from jax.experimental import pallas as pl
from jax.experimental.pallas import tpu as pltpu
from jax.sharding import PartitionSpec as P

HEAD_COUNT = 8
DK = 256
DV = 256
BLOCK = 128
CORES = 2
KEYS, VALUES, QUERIES, GRADS = range(4)
MESH = pl.DeviceIdType.MESH
F32 = jnp.float32
BF16 = jnp.bfloat16


def dot(a, b, ca, cb):
    return lax.dot_general(a, b, (((ca,), (cb,)), ((), ())), preferred_element_type=F32)


def spread_rows(row):
    flat = jnp.broadcast_to(row, (BLOCK, BLOCK))
    return flat, flat.T


def wide(mat, width):
    return jnp.concatenate([mat] * (width // BLOCK), axis=1)


def retention_kernel(
    nx, ny, nz, logs_hbm, q_hbm, k_hbm, v_hbm, g_hbm, gq_ref, gk_ref, gv_ref,
    logs_ref, toks, cum, local, inner, total_buf, from_buf, peer_buf, back_buf,
    chip_buf, x_in, row_tot, y_in, plane_tot, z_in, acc, y_out, row_carry, x_out, carry,
    decay_rows, s_meet, s_logs, s_in, s_core, r_core, s_x, r_x, s_y, r_y, s_z, r_z,
    s_yout, r_yout, s_xout, r_xout, s_back, r_back, s_d, r_d,
):
    count = logs_ref.shape[1] // BLOCK
    scale = DK ** (-0.5)
    half = HEAD_COUNT // CORES
    wx = DK // nx
    wy = wx // ny
    d_core, d_mate = decay_rows.at[0], decay_rows.at[1]
    d_x, d_y = decay_rows.at[pl.ds(2, nx)], decay_rows.at[pl.ds(2 + nx, ny)]
    d_z = decay_rows.at[pl.ds(2 + nx + ny, nz)]
    chunks = [(d, k) for k in range(half) for d in range(2)]
    grp, mem = lax.axis_index("grp"), lax.axis_index("mem")
    z, y = grp // ny, lax.rem(grp, ny)
    x, core = mem // CORES, lax.rem(mem, CORES)
    mate = (grp, x * CORES + 1 - core)

    def x_id(to):
        return (grp, to * CORES + core)

    def y_id(to):
        return (z * ny + to, mem)

    def z_id(to):
        return (to * ny + y, mem)

    xs = [lax.rem(x + off, nx) for off in range(1, nx)]
    ys = [lax.rem(y + off, ny) for off in range(1, ny)]
    zs = [lax.rem(z + off, nz) for off in range(1, nz)]
    barrier = pltpu.get_barrier_semaphore()

    def tell(sem, device):
        pl.semaphore_signal(sem, inc=1, device_id=device, device_id_type=MESH)

    for device in [(grp, o * CORES) for o in xs] + [(z * ny + o, x * CORES) for o in ys]:
        tell(barrier, device)
    pl.when(core == 1)(lambda: tell(barrier, mate))
    for o in zs:
        tell(barrier, (o * ny + y, x * CORES + 1))

    def meet(hearer, signals):
        @pl.when(core == hearer)
        def _():
            pl.semaphore_wait(barrier, signals)
            tell(s_meet, mate)

        @pl.when(core != hearer)
        def _():
            pl.semaphore_wait(s_meet, 1)

    def copy(src, dst, send, recv, device):
        return pltpu.make_async_remote_copy(
            src_ref=src, dst_ref=dst, send_sem=send, recv_sem=recv,
            device_id=device, device_id_type=MESH,
        )

    def go(*args):
        copy(*args).start()

    def landed(ref, sem):
        copy(ref, ref, s_back, sem, mate).wait_recv()

    def left(ref, sem):
        copy(ref, ref, sem, r_back.at[0], mate).wait_send()

    def members(d, size):
        return range(size) if d == 0 else range(size - 1, -1, -1)

    mine, theirs = core * half, (1 - core) * half

    def rows_of(c, size):
        return pl.ds(pl.multiple_of(c * size, size), size)

    def cols_of(head, size):
        return pl.ds(pl.multiple_of(head * size, size), size)

    def tokens_of(b):
        return pl.ds(b * BLOCK, BLOCK)

    load_logs = pltpu.make_async_copy(logs_hbm, logs_ref, s_logs)
    load_logs.start()
    for k in range(half):
        for side, head in enumerate((theirs + k, mine + k)):
            part = cols_of(head, DK)
            for i, far in enumerate((k_hbm, v_hbm, q_hbm, g_hbm)):
                slot = k + 3 if k else 2 * side + i // 2
                pltpu.make_async_copy(
                    far.at[:, part], toks.at[i, :, part], s_in.at[slot]
                ).start()

    def ready(k, slot):
        held = toks.at[:, :, pl.ds(0, CORES * DK)] if k else toks.at[pl.ds(0, 2), :, pl.ds(0, DK)]
        pltpu.make_async_copy(held, held, s_in.at[slot]).wait()

    def tok(i, head, b):
        return toks[i, tokens_of(b), cols_of(head, DK)]

    load_logs.wait()
    carried = None
    for b in range(count):
        row = logs_ref[:, b * BLOCK:(b + 1) * BLOCK]
        lane = lax.broadcasted_iota(jnp.int32, row.shape, 1)
        step = 1
        while step < BLOCK:
            row = row + jnp.where(lane >= step, pltpu.roll(row, step, 1), 0.0)
            step *= 2
        whole = jnp.exp(row[:, BLOCK - 1:BLOCK])
        carried = whole if carried is None else carried * whole
        for h in range(HEAD_COUNT):
            cum[b, h] = row[h:h + 1, :]
    carried = jnp.broadcast_to(carried, (HEAD_COUNT, DV))
    for h in range(HEAD_COUNT):
        d_core[h] = carried[h:h + 1, :]

    def factors(head, b):
        row = cum[b, head]
        flat, cols = spread_rows(row)
        end = row[:, BLOCK - 1:BLOCK]
        return flat, cols, end

    def forward_total(head):
        forward = None
        for b in range(count):
            _, cols, end = factors(head, b)
            kd = tok(KEYS, head, b).astype(F32) * wide(jnp.exp(end - cols), DK)
            whole = jnp.broadcast_to(jnp.exp(end), (1, DV))
            part = dot(kd.astype(BF16), tok(VALUES, head, b), 0, 0)
            if b > 0:
                local[0, b - 1, head] = forward
            forward = part if forward is None else whole * forward + part
        total_buf[0, head] = forward

    def reverse_total(head):
        back = None
        for b in reversed(range(count)):
            _, cols, end = factors(head, b)
            qd = tok(QUERIES, head, b).astype(F32) * wide(jnp.exp(cols), DK)
            whole = jnp.broadcast_to(jnp.exp(end), (1, DV))
            part = dot(qd.astype(BF16), tok(GRADS, head, b), 0, 0)
            if b < count - 1:
                local[1, b, head] = back
            back = part if back is None else whole * back + part
        total_buf[1, head] = back

    lower = lax.broadcasted_iota(jnp.int32, (BLOCK, BLOCK), 0) >= lax.broadcasted_iota(
        jnp.int32, (BLOCK, BLOCK), 1
    )

    def intra(head):
        for b in range(count):
            flat, cols, _ = factors(head, b)
            decay = jnp.where(lower, jnp.exp(jnp.where(lower, cols - flat, 0.0)), 0.0)
            q, k = tok(QUERIES, head, b), tok(KEYS, head, b)
            v, g = tok(VALUES, head, b), tok(GRADS, head, b)
            wg = (dot(g, v, 1, 1) * decay).astype(BF16)
            wv = (dot(q, k, 1, 1) * decay).astype(BF16)
            inner[0, head, tokens_of(b), :] = dot(wg, k, 1, 0)
            inner[1, head, tokens_of(b), :] = dot(wg, q, 0, 0)
            inner[2, head, tokens_of(b), :] = dot(wv, g, 0, 0)

    def outer(d, head):
        coming = from_buf[d, head]
        weight = None
        for step, b in enumerate(members(d, count)):
            _, cols, end = factors(head, b)
            if step == 0:
                low = coming.astype(BF16)
            else:
                low = (local[d, b - 1 if d == 0 else b, head] + weight * coming).astype(BF16)
            whole = jnp.broadcast_to(jnp.exp(end), (1, DV))
            weight = whole if weight is None else weight * whole
            if d == 0:
                far = wide(jnp.exp(cols), DK) * dot(tok(GRADS, head, b), low, 1, 1)
                near = inner[0, head, tokens_of(b), :]
                gq_ref[tokens_of(b), cols_of(head, DK)] = (scale * (near + far)).astype(BF16)
            else:
                tail = wide(jnp.exp(end - cols), DK)
                near = inner[1, head, tokens_of(b), :]
                far = tail * dot(tok(VALUES, head, b), low, 1, 1)
                gk_ref[tokens_of(b), cols_of(head, DK)] = (scale * (near + far)).astype(BF16)
                near = inner[2, head, tokens_of(b), :]
                far = tail * dot(tok(KEYS, head, b), low, 1, 0)
                gv_ref[tokens_of(b), cols_of(head, DV)] = (scale * (near + far)).astype(BF16)

    first = core == 0

    def send_core(n, d, j):
        go(total_buf.at[d, theirs + j], peer_buf.at[d, j], s_core, r_core.at[n], mate)

    def join_cores(n, d, j):
        landed(peer_buf.at[d, j], r_core.at[n])
        own_d, peer_d = d_core[mine + j], d_mate[mine + j]
        one = jnp.ones_like(own_d)
        if d == 0:
            w_own, w_peer = jnp.where(first, peer_d, one), jnp.where(first, one, own_d)
        else:
            w_own, w_peer = jnp.where(first, one, peer_d), jnp.where(first, own_d, one)
        chip_buf[d, j] = w_own * total_buf[d, mine + j] + w_peer * peer_buf[d, j]
        for o in xs:
            go(chip_buf.at[d, j, rows_of(o, wx), :], x_in.at[x, d, j], s_x, r_x.at[n], x_id(o))
        x_in[x, d, j] = chip_buf[d, j, rows_of(x, wx), :]

    def fold(d, j, parts, decays, size):
        running = None
        for c in members(d, size):
            part = parts[c, d, j]
            running = part if running is None else decays[c, mine + j] * running + part
        return running

    def up_x(n, d, j):
        if n == 0:
            landed(d_x.at[pl.ds(0, nx - 1)], r_d.at[1])
            product = d_x[0]
            for c in range(1, nx):
                product = product * d_x[c]
            d_y[y] = product
            for o in ys:
                go(d_y.at[y], d_y.at[y], s_d, r_d.at[2], y_id(o))
        landed(x_in.at[pl.ds(0, nx - 1), d, j], r_x.at[n])
        row_tot[d, j] = fold(d, j, x_in, d_x, nx)
        for o in ys:
            go(row_tot.at[d, j, rows_of(o, wy), :], y_in.at[y, d, j], s_y, r_y.at[n], y_id(o))
        y_in[y, d, j] = row_tot[d, j, rows_of(y, wy), :]

    def up_y(n, d, j):
        if n == 0:
            if ny > 1:
                landed(d_y.at[pl.ds(0, ny - 1)], r_d.at[2])
            product = d_y[0]
            for c in range(1, ny):
                product = product * d_y[c]
            d_z[z] = product
            if nz > 1:
                meet(1, CORES * (nz - 1))
            for t in zs:
                go(d_z.at[z], d_z.at[z], s_d, r_d.at[3], z_id(t))
        if ny > 1:
            landed(y_in.at[pl.ds(0, ny - 1), d, j], r_y.at[n])
        plane_tot[d, j] = fold(d, j, y_in, d_y, ny)
        for t in zs:
            c = copy(plane_tot.at[d, j], z_in.at[z, d, j], s_z, r_z.at[n], z_id(t))
            pl.when((t > z) if d == 0 else (t < z))(c.start)

    def spread(d, j, held, parts, decays, size, out):
        last = members(d, size)[-1]
        for c in members(d, size):
            out[c, d, j] = held
            if c != last:
                held = decays[c, mine + j] * held + parts[c, d, j]

    def over_z(n, d, j):
        if n == 0 and nz > 1:
            landed(d_z.at[pl.ds(0, nz - 1)], r_d.at[3])
        acc[...] = jnp.zeros((wy, DV), F32)
        for coming in range(1, nz):
            @pl.when((z if d == 0 else nz - 1 - z) == coming)
            def _():
                landed(z_in.at[pl.ds(0, coming), d, j], r_z.at[n])
        for t in members(d, nz):
            @pl.when((t < z) if d == 0 else (t > z))
            def _():
                acc[...] = d_z[t, mine + j] * acc[...] + z_in[t, d, j]
        spread(d, j, acc[...], y_in, d_y, ny, y_out)

    def send_y(n, d, j):
        for o in ys:
            go(y_out.at[o, d, j], row_carry.at[d, j, rows_of(y, wy), :], s_yout, r_yout.at[n], y_id(o))
        row_carry[d, j, rows_of(y, wy), :] = y_out[y, d, j]

    def down_y(n, d, j):
        if ny > 1:
            landed(row_carry.at[d, j, pl.ds(0, (ny - 1) * wy), :], r_yout.at[n])
        spread(d, j, row_carry[d, j], x_in, d_x, nx, x_out)
        for o in xs:
            go(x_out.at[o, d, j], carry.at[d, j, rows_of(x, wx), :], s_xout, r_xout.at[n], x_id(o))
        carry[d, j, rows_of(x, wx), :] = x_out[x, d, j]

    def down_x(n, d, j):
        landed(carry.at[d, j, pl.ds(0, (nx - 1) * wx), :], r_xout.at[n])
        near = first if d == 0 else jnp.logical_not(first)

        @pl.when(near)
        def _():
            got = carry[d, j]
            back_buf[d, j] = d_core[mine + j] * got + total_buf[d, mine + j]
            from_buf[d, mine + j] = got

        @pl.when(jnp.logical_not(near))
        def _():
            got = carry[d, j]
            back_buf[d, j] = got
            from_buf[d, mine + j] = d_mate[mine + j] * got + peer_buf[d, j]

        go(back_buf.at[d, j], from_buf.at[d, mine + j], s_back, r_back.at[n], mate)
        outer(d, mine + j)

    def finish(n, d, j):
        landed(from_buf.at[d, theirs + j], r_back.at[n])
        outer(d, theirs + j)

    todo = []
    for k in range(half):
        todo += [
            (forward_total, theirs + k, 2 * k), (reverse_total, theirs + k, 2 * k + 1),
            (forward_total, mine + k, None), (reverse_total, mine + k, None),
        ]
    after = {}
    for n in range(len(chunks)):
        after[min(4 * (n // 2) + 3 + n % 2, len(todo) - 1 + n % 2)] = n
    for i, (work, head, n) in enumerate(todo):
        if i < 4:
            ready(0, i)
        elif i % 4 == 0:
            ready(i // 4, i // 4 + 3)
        work(head)
        if i == 0:
            meet(0, 1 + CORES * (nx + ny - 2))
            go(d_core, d_mate, s_d, r_d.at[0], mate)
        if n is not None:
            send_core(n, *chunks[n])
        if i in after:
            m = after[i]
            if m == 0:
                landed(d_mate, r_d.at[0])
                d_x[x] = d_core[...] * d_mate[...]
                for o in xs:
                    go(d_x.at[x], d_x.at[x], s_d, r_d.at[1], x_id(o))
            join_cores(m, *chunks[m])
    for i in sorted(after):
        if i >= len(todo):
            join_cores(after[i], *chunks[after[i]])

    stages = ((0, up_x), (1, up_y), (3, over_z), (3, send_y), (4, down_y))
    for slot in range(len(chunks) + 4):
        for lag, stage in stages:
            n = slot - lag
            if 0 <= n < len(chunks):
                stage(n, *chunks[n])
            if lag == 0:
                for h in range(slot, HEAD_COUNT, len(chunks)) if slot < len(chunks) else ():
                    intra(h)
    for n, (d, j) in enumerate(chunks):
        down_x(n, d, j)
        if n > 0:
            finish(n - 1, *chunks[n - 1])
    finish(len(chunks) - 1, *chunks[-1])

    left(peer_buf, s_core)
    left(x_in.at[pl.ds(0, nx - 1)], s_x)
    left(x_out.at[pl.ds(0, nx - 1)], s_xout)
    left(back_buf, s_back)
    left(decay_rows.at[pl.ds(0, nx + ny + nz - 2)], s_d)
    if ny > 1:
        left(y_in.at[pl.ds(0, ny - 1)], s_y)
        left(y_out.at[pl.ds(0, ny - 1)], s_yout)
    if nz > 1:
        left(z_in.at[pl.ds(0, nz - 1), 0], s_z)


def write_kernel(gq_ref, gk_ref, gv_ref, gq_hbm, gk_hbm, gv_hbm, sems):
    copies = [
        pltpu.make_async_copy(near, far, sems.at[i])
        for i, (near, far) in enumerate(((gq_ref, gq_hbm), (gk_ref, gk_hbm), (gv_ref, gv_hbm)))
    ]
    for c in copies:
        c.start()
    for c in copies:
        c.wait()


def body(nx, ny, nz, queries, keys, values, grad_out, log_decay):
    tokens = queries.shape[0]
    count = tokens // BLOCK
    half = HEAD_COUNT // CORES
    wx = DK // nx
    wy = wx // ny
    n = 2 * half
    vm = pl.BlockSpec(memory_space=pltpu.VMEM)
    hbm = pl.BlockSpec(memory_space=pltpu.HBM)
    dma = pltpu.SemaphoreType.DMA

    def states(*lead):
        return pltpu.VMEM(lead + (DV,), F32)

    def decays(*lead):
        return pltpu.VMEM(lead + (HEAD_COUNT, 1, DV), F32)

    out = jax.ShapeDtypeStruct((tokens, HEAD_COUNT * DK), BF16)
    near = pltpu.VMEM(out.shape, out.dtype)
    grads = pl.pallas_call(
        functools.partial(retention_kernel, nx, ny, nz),
        out_shape=(near, near, near),
        in_specs=[hbm] * 5,
        out_specs=(vm, vm, vm),
        scratch_shapes=[
            pltpu.VMEM((HEAD_COUNT, tokens), F32),
            pltpu.VMEM((4, tokens, HEAD_COUNT * DK), BF16),
            pltpu.VMEM((count, HEAD_COUNT, 1, BLOCK), F32),
            states(2, max(1, count - 1), HEAD_COUNT, DK),
            states(3, HEAD_COUNT, tokens),
            states(2, HEAD_COUNT, DK), states(2, HEAD_COUNT, DK),
            states(2, half, DK), states(2, half, DK),
            states(2, half, DK), states(nx, 2, half, wx), states(2, half, wx),
            states(ny, 2, half, wy), states(2, half, wy), states(nz, 2, half, wy), states(wy),
            states(ny, 2, half, wy), states(2, half, wx),
            states(nx, 2, half, wx), states(2, half, DK),
            decays(2 + nx + ny + nz), pltpu.SemaphoreType.REGULAR, dma, dma((half + 3,)),
            dma, dma((n,)), dma, dma((n,)), dma, dma((n,)), dma, dma((n,)),
            dma, dma((n,)), dma, dma((n,)), dma, dma((n,)), dma, dma((4,)),
        ],
        compiler_params=pltpu.CompilerParams(collective_id=0, has_side_effects=True, vmem_limit_bytes=52 << 20),
        name="retention",
    )(pltpu.with_memory_space_constraint(log_decay, pltpu.HBM), queries, keys, values, grad_out)
    return pl.pallas_call(
        write_kernel,
        out_shape=(out, out, out),
        in_specs=[vm] * 3,
        out_specs=(hbm, hbm, hbm),
        scratch_shapes=[dma((3,))],
        name="write",
    )(*(pltpu.with_memory_space_constraint(g, pltpu.VMEM) for g in grads))


def solution(mesh):
    nx = mesh.shape["mem"] // CORES
    ny = nx if mesh.shape["grp"] % nx == 0 else 1
    nz = mesh.shape["grp"] // ny
    tokens = P(("grp", "mem"), None)
    return jax.shard_map(
        functools.partial(body, nx, ny, nz),
        mesh=mesh,
        in_specs=(tokens, tokens, tokens, tokens, P(None, ("grp", "mem"))),
        out_specs=(tokens, tokens, tokens),
        check_vma=False,
    )
```

```python
import functools

import jax
import jax.numpy as jnp
from jax import lax
from jax.experimental import pallas as pl
from jax.experimental.pallas import tpu as pltpu
from jax.sharding import PartitionSpec as P

HEAD_COUNT = 8
DK = 256
DV = 256
BLOCK = 128
CORES = 2
KEYS, VALUES, QUERIES, GRADS = range(4)
MESH = pl.DeviceIdType.MESH
F32 = jnp.float32
BF16 = jnp.bfloat16


def dot(a, b, ca, cb):
    return lax.dot_general(a, b, (((ca,), (cb,)), ((), ())), preferred_element_type=F32)


def spread_rows(row):
    flat = jnp.broadcast_to(row, (BLOCK, BLOCK))
    return flat, flat.T


def wide(mat, width):
    return jnp.concatenate([mat] * (width // BLOCK), axis=1)


def retention_kernel(
    nx, ny, nz, logs_hbm, q_hbm, k_hbm, v_hbm, g_hbm, gq_ref, gk_ref, gv_ref,
    logs_ref, toks, cum, local, inner, total_buf, from_buf, peer_buf, back_buf,
    chip_buf, x_in, row_tot, y_in, plane_tot, z_in, z_out, z_carry, y_out, row_carry, x_out, carry,
    decay_rows, weights, s_meet, s_logs, s_in, s_core, r_core, r_first, s_x, r_x, s_y, r_y, s_z, r_z,
    s_yout, r_yout, s_xout, r_xout, s_back, r_back, s_d, r_d,
):
    count = logs_ref.shape[1] // BLOCK
    scale = DK ** (-0.5)
    half = HEAD_COUNT // CORES
    wx = DK // nx
    wy = wx // ny
    d_core, d_mate = decay_rows.at[0], decay_rows.at[1]
    d_x, d_y = decay_rows.at[pl.ds(2, nx)], decay_rows.at[pl.ds(2 + nx, ny)]
    d_z = decay_rows.at[pl.ds(2 + nx + ny, nz)]
    chunks = [(d, k) for k in range(half) for d in range(2)]
    grp, mem = lax.axis_index("grp"), lax.axis_index("mem")
    z, y = grp // ny, lax.rem(grp, ny)
    x, core = mem // CORES, lax.rem(mem, CORES)
    mate = (grp, x * CORES + 1 - core)

    def x_id(to):
        return (grp, to * CORES + core)

    def y_id(to):
        return (z * ny + to, mem)

    def z_id(to):
        return (to * ny + y, mem)

    xs = [lax.rem(x + off, nx) for off in range(1, nx)]
    ys = [lax.rem(y + off, ny) for off in range(1, ny)]
    zs = [lax.rem(z + off, nz) for off in range(1, nz)]
    barrier = pltpu.get_barrier_semaphore()

    def tell(sem, device):
        pl.semaphore_signal(sem, inc=1, device_id=device, device_id_type=MESH)

    for device in [(grp, o * CORES) for o in xs] + [(z * ny + o, x * CORES) for o in ys]:
        tell(barrier, device)
    pl.when(core == 1)(lambda: tell(barrier, mate))
    for o in zs:
        tell(barrier, (o * ny + y, x * CORES + 1))

    def hear(hearer, signals):
        @pl.when(core == hearer)
        def _():
            pl.semaphore_wait(barrier, signals)
            tell(s_meet, mate)

    def learn(hearer):
        @pl.when(core != hearer)
        def _():
            pl.semaphore_wait(s_meet, 1)

    def copy(src, dst, send, recv, device):
        return pltpu.make_async_remote_copy(
            src_ref=src, dst_ref=dst, send_sem=send, recv_sem=recv,
            device_id=device, device_id_type=MESH,
        )

    def go(*args):
        copy(*args).start()

    def landed(ref, sem):
        copy(ref, ref, s_back, sem, mate).wait_recv()

    def left(ref, sem):
        copy(ref, ref, sem, r_back.at[0], mate).wait_send()

    def members(d, size):
        return range(size) if d == 0 else range(size - 1, -1, -1)

    mine, theirs = core * half, (1 - core) * half

    def rows_of(c, size):
        return pl.ds(pl.multiple_of(c * size, size), size)

    def cols_of(head, size):
        return pl.ds(pl.multiple_of(head * size, size), size)

    def tokens_of(b):
        return pl.ds(b * BLOCK, BLOCK)

    load_logs = pltpu.make_async_copy(logs_hbm, logs_ref, s_logs)
    load_logs.start()

    def load(k):
        for side, head in enumerate((theirs + k, mine + k)):
            part = cols_of(head, DK)
            for i, far in enumerate((k_hbm, v_hbm, q_hbm, g_hbm)):
                slot = k + 3 if k else 2 * side + i // 2
                pltpu.make_async_copy(
                    far.at[:, part], toks.at[i, :, part], s_in.at[slot]
                ).start()

    load(0)

    def ready(k, slot):
        held = toks.at[:, :, pl.ds(0, CORES * DK)] if k else toks.at[pl.ds(0, 2), :, pl.ds(0, DK)]
        pltpu.make_async_copy(held, held, s_in.at[slot]).wait()

    def tok(i, head, b):
        return toks[i, tokens_of(b), cols_of(head, DK)]

    square = (BLOCK, BLOCK)
    lower = lax.broadcasted_iota(jnp.int32, square, 0) >= lax.broadcasted_iota(jnp.int32, square, 1)
    ones = jnp.where(lower, 1.0, 0.0)
    load_logs.wait()
    carried = None
    for b in range(count):
        row = lax.dot_general(
            logs_ref[:, b * BLOCK:(b + 1) * BLOCK], ones, (((1,), (1,)), ((), ())),
            precision=lax.Precision.HIGHEST, preferred_element_type=F32,
        )
        for h in range(HEAD_COUNT):
            cum[b, h] = row[h:h + 1, :]
        whole = jnp.exp(row[:, BLOCK - 1:BLOCK])
        carried = whole if carried is None else carried * whole
    carried = jnp.broadcast_to(carried, (HEAD_COUNT, DV))
    for h in range(HEAD_COUNT):
        d_core[h] = carried[h:h + 1, :]
    hear(0, 1 + CORES * (nx + ny - 2))

    def factors(head, b):
        row = cum[b, head]
        flat, cols = spread_rows(row)
        end = row[:, BLOCK - 1:BLOCK]
        return flat, cols, end

    def forward_total(head):
        forward = None
        for b in range(count):
            _, cols, end = factors(head, b)
            kd = tok(KEYS, head, b).astype(F32) * wide(jnp.exp(end - cols), DK)
            whole = jnp.broadcast_to(jnp.exp(end), (1, DV))
            part = dot(kd.astype(BF16), tok(VALUES, head, b), 0, 0)
            if b > 0:
                local[0, b - 1, head] = forward
            forward = part if forward is None else whole * forward + part
        total_buf[0, head] = forward

    def reverse_total(head):
        back = None
        for b in reversed(range(count)):
            _, cols, end = factors(head, b)
            qd = tok(QUERIES, head, b).astype(F32) * wide(jnp.exp(cols), DK)
            whole = jnp.broadcast_to(jnp.exp(end), (1, DV))
            part = dot(qd.astype(BF16), tok(GRADS, head, b), 0, 0)
            if b < count - 1:
                local[1, b, head] = back
            back = part if back is None else whole * back + part
        total_buf[1, head] = back

    def intra(head):
        for b in range(count):
            flat, cols, _ = factors(head, b)
            decay = jnp.where(lower, jnp.exp(jnp.where(lower, cols - flat, 0.0)), 0.0)
            q, k = tok(QUERIES, head, b), tok(KEYS, head, b)
            v, g = tok(VALUES, head, b), tok(GRADS, head, b)
            wg = (dot(g, v, 1, 1) * decay).astype(BF16)
            wv = (dot(q, k, 1, 1) * decay).astype(BF16)
            inner[0, head, tokens_of(b), :] = dot(wg, k, 1, 0)
            inner[1, head, tokens_of(b), :] = dot(wg, q, 0, 0)
            inner[2, head, tokens_of(b), :] = dot(wv, g, 0, 0)

    def outer(d, head):
        coming = from_buf[d, head]
        weight = None
        for step, b in enumerate(members(d, count)):
            _, cols, end = factors(head, b)
            if step == 0:
                low = coming.astype(BF16)
            else:
                low = (local[d, b - 1 if d == 0 else b, head] + weight * coming).astype(BF16)
            whole = jnp.broadcast_to(jnp.exp(end), (1, DV))
            weight = whole if weight is None else weight * whole
            if d == 0:
                far = wide(jnp.exp(cols), DK) * dot(tok(GRADS, head, b), low, 1, 1)
                near = inner[0, head, tokens_of(b), :]
                gq_ref[tokens_of(b), cols_of(head, DK)] = (scale * (near + far)).astype(BF16)
            else:
                tail = wide(jnp.exp(end - cols), DK)
                near = inner[1, head, tokens_of(b), :]
                far = tail * dot(tok(VALUES, head, b), low, 1, 1)
                gk_ref[tokens_of(b), cols_of(head, DK)] = (scale * (near + far)).astype(BF16)
                near = inner[2, head, tokens_of(b), :]
                far = tail * dot(tok(KEYS, head, b), low, 1, 0)
                gv_ref[tokens_of(b), cols_of(head, DV)] = (scale * (near + far)).astype(BF16)

    first = core == 0

    def send_core(n, d, j):
        if n:
            go(total_buf.at[d, theirs + j], peer_buf.at[d, j], s_core, r_core.at[n], mate)
        else:
            for i, o in enumerate(xs + [x]):
                part = rows_of(o, wx)
                go(total_buf.at[d, theirs + j, part, :], peer_buf.at[d, j, part, :],
                   s_core, r_first.at[i], mate)

    def join_cores(n, d, j):
        if n:
            landed(peer_buf.at[d, j], r_core.at[n])
        own_d, peer_d = d_core[mine + j], d_mate[mine + j]
        one = jnp.ones_like(own_d)
        if d == 0:
            w_own, w_peer = jnp.where(first, peer_d, one), jnp.where(first, one, own_d)
        else:
            w_own, w_peer = jnp.where(first, one, peer_d), jnp.where(first, own_d, one)

        def joined(o):
            part = rows_of(o, wx)
            return w_own * total_buf[d, mine + j, part, :] + w_peer * peer_buf[d, j, part, :]

        for i, o in enumerate(xs):
            if n == 0:
                landed(peer_buf.at[d, j, rows_of(o, wx), :], r_first.at[i])
            chip_buf[d, j, rows_of(o, wx), :] = joined(o)
            go(chip_buf.at[d, j, rows_of(o, wx), :], x_in.at[x, d, j], s_x, r_x.at[n], x_id(o))
        if n == 0:
            landed(peer_buf.at[d, j, rows_of(x, wx), :], r_first.at[nx - 1])
        x_in[x, d, j] = joined(x)

    def fold(d, j, parts, decays, size):
        running = None
        for c in members(d, size):
            part = parts[c, d, j]
            running = part if running is None else decays[c, mine + j] * running + part
        return running

    def up_x(n, d, j):
        if n == 0:
            landed(d_x.at[pl.ds(0, nx - 1)], r_d.at[1])
            product = d_x[0]
            for c in range(1, nx):
                product = product * d_x[c]
            d_y[y] = product
            for o in ys:
                go(d_y.at[y], d_y.at[y], s_d, r_d.at[2], y_id(o))
        landed(x_in.at[pl.ds(0, nx - 1), d, j], r_x.at[n])
        row_tot[d, j] = fold(d, j, x_in, d_x, nx)
        for o in ys:
            go(row_tot.at[d, j, rows_of(o, wy), :], y_in.at[y, d, j], s_y, r_y.at[n], y_id(o))
        y_in[y, d, j] = row_tot[d, j, rows_of(y, wy), :]

    def up_y(n, d, j):
        if n == 0:
            if ny > 1:
                landed(d_y.at[pl.ds(0, ny - 1)], r_d.at[2])
            product = d_y[0]
            for c in range(1, ny):
                product = product * d_y[c]
            d_z[z] = product
            if nz > 1:
                hear(1, CORES * (nz - 1))
                learn(1)
            for t in zs:
                go(d_z.at[z], d_z.at[z], s_d, r_d.at[3], z_id(t))
        if ny > 1:
            landed(y_in.at[pl.ds(0, ny - 1), d, j], r_y.at[n])
        plane_tot[d, j] = fold(d, j, y_in, d_y, ny)
        send_z(n, d, j, 0, plane_tot.at[d, j])

    levels = (nz - 1).bit_length()

    def place(d):
        return z if d == 0 else nz - 1 - z

    def z_sends(d, level):
        size, p = 1 << level, place(d)
        last = lax.rem(p, 2 * size) == size - 1
        return [(i + 1, jnp.logical_and(last, p + i + 1 < nz)) for i in range(size)]

    def z_hears(d, level):
        return lax.rem(place(d), 2 << level) >= 1 << level

    def send_z(n, d, j, level, src):
        if level < levels:
            for hop, needed in z_sends(d, level):
                to = lax.rem(z + hop, nz) if d == 0 else lax.rem(z - hop + nz, nz)
                c = copy(src, z_in.at[2 * level + d, j], s_z, r_z.at[level, n], z_id(to))
                pl.when(needed)(c.start)

    def z_weight(d, level):
        size = 1 << level
        start = place(d) // size * size
        weight = jnp.ones_like(d_core[...])
        for i in range(size - 1):
            q = lax.rem(start + i, nz)
            passed = d_z[q if d == 0 else nz - 1 - q]
            weight = jnp.where(start + i < place(d), weight * passed, weight)
        return weight

    def spread(d, j, held, parts, decays, size, out):
        last = members(d, size)[-1]
        for c in members(d, size):
            out[c, d, j] = held
            if c != last:
                held = decays[c, mine + j] * held + parts[c, d, j]

    def over_z(level, n, d, j):
        if n == 0 and level == 0:
            landed(d_z.at[pl.ds(0, nz - 1)], r_d.at[3])
            for side in range(2):
                for upper in range(levels):
                    weights[upper, side] = z_weight(side, upper)
        if level == 0:
            z_carry[d, j] = jnp.zeros((wy, DV), F32)

        @pl.when(z_hears(d, level))
        def _():
            landed(z_in.at[2 * level + d, j], r_z.at[level, n])
            came = z_in[2 * level + d, j]
            if level:
                came = weights[level, d, mine + j] * came + z_carry[d, j]
            z_carry[d, j] = came

        if level + 1 < levels:
            @pl.when(z_sends(d, level + 1)[0][1])
            def _():
                z_out[level, d, j] = d_z[z, mine + j] * z_carry[d, j] + plane_tot[d, j]

            send_z(n, d, j, level + 1, z_out.at[level, d, j])

    def down_z(n, d, j):
        if levels:
            over_z(levels - 1, n, d, j)
        else:
            z_carry[d, j] = jnp.zeros((wy, DV), F32)
        spread(d, j, z_carry[d, j], y_in, d_y, ny, y_out)
        send_y(n, d, j)

    def send_y(n, d, j):
        for o in ys:
            go(y_out.at[o, d, j], row_carry.at[d, j, rows_of(y, wy), :], s_yout, r_yout.at[n], y_id(o))
        row_carry[d, j, rows_of(y, wy), :] = y_out[y, d, j]

    def starts(d, at):
        row = jnp.logical_and(z == (0 if d == 0 else nz - 1), y == (0 if d == 0 else ny - 1))
        return jnp.logical_and(row, at == (0 if d == 0 else nx - 1))

    def down_y(n, d, j):
        if ny > 1:
            landed(row_carry.at[d, j, pl.ds(0, (ny - 1) * wy), :], r_yout.at[n])
        spread(d, j, row_carry[d, j], x_in, d_x, nx, x_out)
        for o in xs:
            c = copy(
                x_out.at[o, d, j], carry.at[d, j, rows_of(x, wx), :], s_xout.at[d], r_xout.at[n], x_id(o)
            )
            pl.when(jnp.logical_not(starts(d, o)))(c.start)
        carry[d, j, rows_of(x, wx), :] = x_out[x, d, j]

    def down_x(n, d, j):
        starting = starts(d, x)

        @pl.when(starting)
        def _():
            carry[d, j] = jnp.zeros((DK, DV), F32)

        @pl.when(jnp.logical_not(starting))
        def _():
            landed(carry.at[d, j, pl.ds(0, (nx - 1) * wx), :], r_xout.at[n])

        near = first if d == 0 else jnp.logical_not(first)

        @pl.when(near)
        def _():
            got = carry[d, j]
            back_buf[d, j] = d_core[mine + j] * got + total_buf[d, mine + j]
            from_buf[d, mine + j] = got

        @pl.when(jnp.logical_not(near))
        def _():
            got = carry[d, j]
            back_buf[d, j] = got
            from_buf[d, mine + j] = d_mate[mine + j] * got + peer_buf[d, j]

        go(back_buf.at[d, j], from_buf.at[d, mine + j], s_back, r_back.at[n], mate)
        outer(d, mine + j)

    def finish(n, d, j):
        landed(from_buf.at[d, theirs + j], r_back.at[n])
        outer(d, theirs + j)

    todo = []
    for k in range(half):
        todo += [
            (forward_total, theirs + k, 2 * k), (reverse_total, theirs + k, 2 * k + 1),
            (forward_total, mine + k, None), (reverse_total, mine + k, None),
        ]
    after = {}
    for n in range(len(chunks)):
        after[min(4 * (n // 2) + 3 + n % 2, len(todo) - 1 + n % 2)] = n
    for i, (work, head, n) in enumerate(todo):
        if i < 4:
            ready(0, i)
        elif i % 4 == 0:
            ready(i // 4, i // 4 + 3)
        work(head)
        if i == 0:
            learn(0)
            go(d_core, d_mate, s_d, r_d.at[0], mate)
            for k in range(1, half):
                load(k)
        if n is not None:
            send_core(n, *chunks[n])
        if i in after:
            m = after[i]
            if m == 0:
                landed(d_mate, r_d.at[0])
                d_x[x] = d_core[...] * d_mate[...]
                for o in xs:
                    go(d_x.at[x], d_x.at[x], s_d, r_d.at[1], x_id(o))
            join_cores(m, *chunks[m])
    for i in sorted(after):
        if i >= len(todo):
            join_cores(after[i], *chunks[after[i]])

    def inside(n, d, j):
        for h in range(n, HEAD_COUNT, len(chunks)):
            intra(h)

    climb = [(2 + level, functools.partial(over_z, level)) for level in range(levels - 1)]
    top = 2 + len(climb)
    back = len(chunks)
    stages = [(0, up_x), (0, inside), (top + 2, down_y), (back + 1, finish), (back, down_x)]
    stages += [(1, up_y)] + climb + [(top, down_z)]
    for slot in range(2 * len(chunks) + 1):
        for lag, stage in stages:
            n = slot - lag
            if 0 <= n < len(chunks):
                stage(n, *chunks[n])

    left(peer_buf, s_core)
    left(x_in.at[pl.ds(0, nx - 1)], s_x)
    withheld = [
        sum(jnp.where(starts(d, o), 1, 0) for o in xs) for d in range(2)
    ]
    for d in range(2):
        for amount in (nx - 2, nx - 1):
            if amount:
                pl.when(withheld[d] == nx - 1 - amount)(
                    functools.partial(left, x_out.at[pl.ds(0, amount), d], s_xout.at[d])
                )
    left(back_buf, s_back)
    left(decay_rows.at[pl.ds(0, nx + ny + nz - 2)], s_d)
    if ny > 1:
        left(y_in.at[pl.ds(0, ny - 1)], s_y)
        left(y_out.at[pl.ds(0, ny - 1)], s_yout)
    if nz > 1:
        sends = sum(
            jnp.where(needed, 1, 0)
            for level in range(levels) for d in range(2) for _, needed in z_sends(d, level)
        )
        for amount in range(1, nz):
            pl.when(sends == amount)(functools.partial(left, z_in.at[pl.ds(0, amount)], s_z))


def write_kernel(gq_ref, gk_ref, gv_ref, gq_hbm, gk_hbm, gv_hbm, sems):
    copies = [
        pltpu.make_async_copy(near, far, sems.at[i])
        for i, (near, far) in enumerate(((gq_ref, gq_hbm), (gk_ref, gk_hbm), (gv_ref, gv_hbm)))
    ]
    for c in copies:
        c.start()
    for c in copies:
        c.wait()


def body(nx, ny, nz, queries, keys, values, grad_out, log_decay):
    tokens = queries.shape[0]
    count = tokens // BLOCK
    half = HEAD_COUNT // CORES
    wx = DK // nx
    wy = wx // ny
    levels = (nz - 1).bit_length()
    n = 2 * half
    vm = pl.BlockSpec(memory_space=pltpu.VMEM)
    hbm = pl.BlockSpec(memory_space=pltpu.HBM)
    dma = pltpu.SemaphoreType.DMA

    def states(*lead):
        return pltpu.VMEM(lead + (DV,), F32)

    def decays(*lead):
        return pltpu.VMEM(lead + (HEAD_COUNT, 1, DV), F32)

    out = jax.ShapeDtypeStruct((tokens, HEAD_COUNT * DK), BF16)
    near = pltpu.VMEM(out.shape, out.dtype)
    grads = pl.pallas_call(
        functools.partial(retention_kernel, nx, ny, nz),
        out_shape=(near, near, near),
        in_specs=[hbm] * 5,
        out_specs=(vm, vm, vm),
        scratch_shapes=[
            pltpu.VMEM((HEAD_COUNT, tokens), F32),
            pltpu.VMEM((4, tokens, HEAD_COUNT * DK), BF16),
            pltpu.VMEM((count, HEAD_COUNT, 1, BLOCK), F32),
            states(2, max(1, count - 1), HEAD_COUNT, DK),
            states(3, HEAD_COUNT, tokens),
            states(2, HEAD_COUNT, DK), states(2, HEAD_COUNT, DK),
            states(2, half, DK), states(2, half, DK),
            states(2, half, DK), states(nx, 2, half, wx), states(2, half, wx),
            states(ny, 2, half, wy), states(2, half, wy),
            states(max(2 * levels, nz), half, wy), states(max(1, levels - 1), 2, half, wy), states(2, half, wy),
            states(ny, 2, half, wy), states(2, half, wx),
            states(nx, 2, half, wx), states(2, half, DK),
            decays(2 + nx + ny + nz), decays(max(1, levels), 2), pltpu.SemaphoreType.REGULAR, dma, dma((half + 3,)),
            dma, dma((n,)), dma((nx,)), dma, dma((n,)), dma, dma((n,)), dma, dma((max(1, levels), n)),
            dma, dma((n,)), dma((2,)), dma((n,)), dma, dma((n,)), dma, dma((4,)),
        ],
        compiler_params=pltpu.CompilerParams(collective_id=0, has_side_effects=True, vmem_limit_bytes=52 << 20),
        name="retention",
    )(pltpu.with_memory_space_constraint(log_decay, pltpu.HBM), queries, keys, values, grad_out)
    return pl.pallas_call(
        write_kernel,
        out_shape=(out, out, out),
        in_specs=[vm] * 3,
        out_specs=(hbm, hbm, hbm),
        scratch_shapes=[dma((3,))],
        name="write",
    )(*(pltpu.with_memory_space_constraint(g, pltpu.VMEM) for g in grads))


def solution(mesh):
    nx = mesh.shape["mem"] // CORES
    ny = nx if mesh.shape["grp"] % nx == 0 else 1
    nz = mesh.shape["grp"] // ny
    tokens = P(("grp", "mem"), None)
    return jax.shard_map(
        functools.partial(body, nx, ny, nz),
        mesh=mesh,
        in_specs=(tokens, tokens, tokens, tokens, P(None, ("grp", "mem"))),
        out_specs=(tokens, tokens, tokens),
        check_vma=False,
    )
```

```python
import functools

import jax
import jax.numpy as jnp
from jax import lax
from jax.experimental import pallas as pl
from jax.experimental.pallas import tpu as pltpu
from jax.sharding import PartitionSpec as P

HEAD_COUNT = 8
DK = 256
DV = 256
BLOCK = 128
CORES = 2
KEYS, VALUES, QUERIES, GRADS = range(4)
MESH = pl.DeviceIdType.MESH
F32 = jnp.float32
BF16 = jnp.bfloat16


def dot(a, b, ca, cb):
    return lax.dot_general(a, b, (((ca,), (cb,)), ((), ())), preferred_element_type=F32)


def spread_rows(row):
    flat = jnp.broadcast_to(row, (BLOCK, BLOCK))
    return flat, flat.T


def wide(mat, width):
    return jnp.concatenate([mat] * (width // BLOCK), axis=1)


def retention_kernel(
    nx, ny, nz, logs_hbm, q_hbm, k_hbm, v_hbm, g_hbm, gq_ref, gk_ref, gv_ref,
    logs_ref, toks, cum, local, inner, total_buf, from_buf, peer_buf, back_buf,
    chip_buf, x_in, row_tot, y_in, plane_tot, z_in, z_out, z_carry, y_out, row_carry, x_out, carry,
    decay_rows, weights, s_meet, s_logs, s_in, s_core, r_core, r_first, s_x, r_x, s_y, r_y, s_z, r_z,
    s_yout, r_yout, s_xout, r_xout, s_back, r_back, s_d, r_d,
):
    count = logs_ref.shape[1] // BLOCK
    scale = DK ** (-0.5)
    half = HEAD_COUNT // CORES
    wx = DK // nx
    wy = wx // ny
    d_core, d_mate = decay_rows.at[0], decay_rows.at[1]
    d_x, d_y = decay_rows.at[pl.ds(2, nx)], decay_rows.at[pl.ds(2 + nx, ny)]
    d_z = decay_rows.at[pl.ds(2 + nx + ny, nz)]
    chunks = [(d, k) for k in range(half) for d in range(2)]
    chunks[-2:] = chunks[:-3:-1]
    grp, mem = lax.axis_index("grp"), lax.axis_index("mem")
    z, y = grp // ny, lax.rem(grp, ny)
    x, core = mem // CORES, lax.rem(mem, CORES)
    mate = (grp, x * CORES + 1 - core)

    def x_id(to):
        return (grp, to * CORES + core)

    def y_id(to):
        return (z * ny + to, mem)

    def z_id(to):
        return (to * ny + y, mem)

    xs = [lax.rem(x + off, nx) for off in range(1, nx)]
    ys = [lax.rem(y + off, ny) for off in range(1, ny)]
    zs = [lax.rem(z + off, nz) for off in range(1, nz)]
    barrier = pltpu.get_barrier_semaphore()

    def tell(sem, device):
        pl.semaphore_signal(sem, inc=1, device_id=device, device_id_type=MESH)

    for device in [(grp, o * CORES) for o in xs] + [(z * ny + o, x * CORES) for o in ys]:
        tell(barrier, device)
    pl.when(core == 1)(lambda: tell(barrier, mate))
    for o in zs:
        tell(barrier, (o * ny + y, x * CORES + 1))

    def hear(hearer, signals):
        @pl.when(core == hearer)
        def _():
            pl.semaphore_wait(barrier, signals)
            tell(s_meet, mate)

    def learn(hearer):
        @pl.when(core != hearer)
        def _():
            pl.semaphore_wait(s_meet, 1)

    def copy(src, dst, send, recv, device):
        return pltpu.make_async_remote_copy(
            src_ref=src, dst_ref=dst, send_sem=send, recv_sem=recv,
            device_id=device, device_id_type=MESH,
        )

    def go(*args):
        copy(*args).start()

    def landed(ref, sem):
        copy(ref, ref, s_back, sem, mate).wait_recv()

    def left(ref, sem):
        copy(ref, ref, sem, r_back.at[0], mate).wait_send()

    def members(d, size):
        return range(size) if d == 0 else range(size - 1, -1, -1)

    mine, theirs = core * half, (1 - core) * half

    def rows_of(c, size):
        return pl.ds(pl.multiple_of(c * size, size), size)

    def cols_of(head, size):
        return pl.ds(pl.multiple_of(head * size, size), size)

    def tokens_of(b):
        return pl.ds(b * BLOCK, BLOCK)

    load_logs = pltpu.make_async_copy(logs_hbm, logs_ref, s_logs)
    load_logs.start()

    def load(head, pair, slot):
        part = cols_of(head, DK)
        for i in (2 * pair, 2 * pair + 1):
            far = (k_hbm, v_hbm, q_hbm, g_hbm)[i]
            pltpu.make_async_copy(far.at[:, part], toks.at[i, :, part], s_in.at[slot]).start()

    load(theirs, 0, 0)

    def ready(k, slot):
        held = toks.at[:, :, pl.ds(0, CORES * DK)] if k else toks.at[pl.ds(0, 2), :, pl.ds(0, DK)]
        pltpu.make_async_copy(held, held, s_in.at[slot]).wait()

    def tok(i, head, b):
        return toks[i, tokens_of(b), cols_of(head, DK)]

    square = (BLOCK, BLOCK)
    lower = lax.broadcasted_iota(jnp.int32, square, 0) >= lax.broadcasted_iota(jnp.int32, square, 1)
    ones = jnp.where(lower, 1.0, 0.0)
    load_logs.wait()
    for slot, head in ((2, mine), (1, theirs), (3, mine)):
        load(head, slot % 2, slot)
    carried = None
    for b in range(count):
        row = lax.dot_general(
            logs_ref[:, b * BLOCK:(b + 1) * BLOCK], ones, (((1,), (1,)), ((), ())),
            precision=lax.Precision.HIGHEST, preferred_element_type=F32,
        )
        for h in range(HEAD_COUNT):
            cum[b, h] = row[h:h + 1, :]
        whole = jnp.exp(row[:, BLOCK - 1:BLOCK])
        carried = whole if carried is None else carried * whole
    carried = jnp.broadcast_to(carried, (HEAD_COUNT, DV))
    for h in range(HEAD_COUNT):
        d_core[h] = carried[h:h + 1, :]
    def factors(head, b):
        row = cum[b, head]
        flat, cols = spread_rows(row)
        end = row[:, BLOCK - 1:BLOCK]
        return flat, cols, end

    def forward_total(head):
        forward = None
        for b in range(count):
            _, cols, end = factors(head, b)
            kd = tok(KEYS, head, b).astype(F32) * wide(jnp.exp(end - cols), DK)
            whole = jnp.broadcast_to(jnp.exp(end), (1, DV))
            part = dot(kd.astype(BF16), tok(VALUES, head, b), 0, 0)
            if b > 0:
                local[0, b - 1, head] = forward
            forward = part if forward is None else whole * forward + part
        total_buf[0, head] = forward

    def reverse_total(head):
        back = None
        for b in reversed(range(count)):
            _, cols, end = factors(head, b)
            qd = tok(QUERIES, head, b).astype(F32) * wide(jnp.exp(cols), DK)
            whole = jnp.broadcast_to(jnp.exp(end), (1, DV))
            part = dot(qd.astype(BF16), tok(GRADS, head, b), 0, 0)
            if b < count - 1:
                local[1, b, head] = back
            back = part if back is None else whole * back + part
        total_buf[1, head] = back

    def intra(head):
        for b in range(count):
            flat, cols, _ = factors(head, b)
            decay = jnp.where(lower, jnp.exp(jnp.where(lower, cols - flat, 0.0)), 0.0)
            q, k = tok(QUERIES, head, b), tok(KEYS, head, b)
            v, g = tok(VALUES, head, b), tok(GRADS, head, b)
            wg = (dot(g, v, 1, 1) * decay).astype(BF16)
            wv = (dot(q, k, 1, 1) * decay).astype(BF16)
            inner[0, head, tokens_of(b), :] = dot(wg, k, 1, 0)
            inner[1, head, tokens_of(b), :] = dot(wg, q, 0, 0)
            inner[2, head, tokens_of(b), :] = dot(wv, g, 0, 0)

    def outer(d, head):
        coming = from_buf[d, head]
        weight = None
        for step, b in enumerate(members(d, count)):
            _, cols, end = factors(head, b)
            if step == 0:
                low = coming.astype(BF16)
            else:
                low = (local[d, b - 1 if d == 0 else b, head] + weight * coming).astype(BF16)
            whole = jnp.broadcast_to(jnp.exp(end), (1, DV))
            weight = whole if weight is None else weight * whole
            if d == 0:
                far = wide(jnp.exp(cols), DK) * dot(tok(GRADS, head, b), low, 1, 1)
                near = inner[0, head, tokens_of(b), :]
                gq_ref[tokens_of(b), cols_of(head, DK)] = (scale * (near + far)).astype(BF16)
            else:
                tail = wide(jnp.exp(end - cols), DK)
                near = inner[1, head, tokens_of(b), :]
                far = tail * dot(tok(VALUES, head, b), low, 1, 1)
                gk_ref[tokens_of(b), cols_of(head, DK)] = (scale * (near + far)).astype(BF16)
                near = inner[2, head, tokens_of(b), :]
                far = tail * dot(tok(KEYS, head, b), low, 1, 0)
                gv_ref[tokens_of(b), cols_of(head, DV)] = (scale * (near + far)).astype(BF16)

    first = core == 0

    def send_core(n, d, j):
        if n:
            go(total_buf.at[d, theirs + j], peer_buf.at[d, j], s_core, r_core.at[n], mate)
        else:
            for i, o in enumerate(xs + [x]):
                part = rows_of(o, wx)
                go(total_buf.at[d, theirs + j, part, :], peer_buf.at[d, j, part, :],
                   s_core, r_first.at[i], mate)

    def join_cores(n, d, j):
        if n:
            landed(peer_buf.at[d, j], r_core.at[n])
        own_d, peer_d = d_core[mine + j], d_mate[mine + j]
        one = jnp.ones_like(own_d)
        if d == 0:
            w_own, w_peer = jnp.where(first, peer_d, one), jnp.where(first, one, own_d)
        else:
            w_own, w_peer = jnp.where(first, one, peer_d), jnp.where(first, own_d, one)

        def joined(o):
            part = rows_of(o, wx)
            return w_own * total_buf[d, mine + j, part, :] + w_peer * peer_buf[d, j, part, :]

        for i, o in enumerate(xs):
            if n == 0:
                landed(peer_buf.at[d, j, rows_of(o, wx), :], r_first.at[i])
            chip_buf[d, j, rows_of(o, wx), :] = joined(o)
            go(chip_buf.at[d, j, rows_of(o, wx), :], x_in.at[x, d, j], s_x, r_x.at[n], x_id(o))
        if n == 0:
            landed(peer_buf.at[d, j, rows_of(x, wx), :], r_first.at[nx - 1])
        x_in[x, d, j] = joined(x)

    def fold(d, j, parts, decays, size):
        running = None
        for c in members(d, size):
            part = parts[c, d, j]
            running = part if running is None else decays[c, mine + j] * running + part
        return running

    def up_x(n, d, j):
        if n == 0:
            landed(d_x.at[pl.ds(0, nx - 1)], r_d.at[1])
            product = d_x[0]
            for c in range(1, nx):
                product = product * d_x[c]
            d_y[y] = product
            for o in ys:
                go(d_y.at[y], d_y.at[y], s_d, r_d.at[2], y_id(o))
        landed(x_in.at[pl.ds(0, nx - 1), d, j], r_x.at[n])
        row_tot[d, j] = fold(d, j, x_in, d_x, nx)
        for o in ys:
            go(row_tot.at[d, j, rows_of(o, wy), :], y_in.at[y, d, j], s_y, r_y.at[n], y_id(o))
        y_in[y, d, j] = row_tot[d, j, rows_of(y, wy), :]

    def up_y(n, d, j):
        if n == 0:
            if ny > 1:
                landed(d_y.at[pl.ds(0, ny - 1)], r_d.at[2])
            product = d_y[0]
            for c in range(1, ny):
                product = product * d_y[c]
            d_z[z] = product
            if nz > 1:
                hear(1, CORES * (nz - 1))
                learn(1)
            for t in zs:
                go(d_z.at[z], d_z.at[z], s_d, r_d.at[3], z_id(t))
        if ny > 1:
            landed(y_in.at[pl.ds(0, ny - 1), d, j], r_y.at[n])
        plane_tot[d, j] = fold(d, j, y_in, d_y, ny)
        send_z(n, d, j, 0, plane_tot.at[d, j])

    levels = (nz - 1).bit_length()

    def place(d):
        return z if d == 0 else nz - 1 - z

    def z_sends(d, level):
        size, p = 1 << level, place(d)
        last = lax.rem(p, 2 * size) == size - 1
        return [(i + 1, jnp.logical_and(last, p + i + 1 < nz)) for i in range(size)]

    def z_hears(d, level):
        return lax.rem(place(d), 2 << level) >= 1 << level

    def send_z(n, d, j, level, src):
        if level < levels:
            for hop, needed in z_sends(d, level):
                to = lax.rem(z + hop, nz) if d == 0 else lax.rem(z - hop + nz, nz)
                c = copy(src, z_in.at[2 * level + d, j], s_z, r_z.at[level, n], z_id(to))
                pl.when(needed)(c.start)

    def z_weight(d, level):
        size = 1 << level
        start = place(d) // size * size
        weight = jnp.ones_like(d_core[...])
        for i in range(size - 1):
            q = lax.rem(start + i, nz)
            passed = d_z[q if d == 0 else nz - 1 - q]
            weight = jnp.where(start + i < place(d), weight * passed, weight)
        return weight

    def spread(d, j, held, parts, decays, size, out):
        last = members(d, size)[-1]
        for c in members(d, size):
            out[c, d, j] = held
            if c != last:
                held = decays[c, mine + j] * held + parts[c, d, j]

    def over_z(level, n, d, j):
        if n == 0 and level == 0:
            landed(d_z.at[pl.ds(0, nz - 1)], r_d.at[3])
            for side in range(2):
                for upper in range(levels):
                    weights[upper, side] = z_weight(side, upper)
        if level == 0:
            z_carry[d, j] = jnp.zeros((wy, DV), F32)

        @pl.when(z_hears(d, level))
        def _():
            landed(z_in.at[2 * level + d, j], r_z.at[level, n])
            came = z_in[2 * level + d, j]
            if level:
                came = weights[level, d, mine + j] * came + z_carry[d, j]
            z_carry[d, j] = came

        if level + 1 < levels:
            @pl.when(z_sends(d, level + 1)[0][1])
            def _():
                z_out[level, d, j] = d_z[z, mine + j] * z_carry[d, j] + plane_tot[d, j]

            send_z(n, d, j, level + 1, z_out.at[level, d, j])

    def down_z(n, d, j):
        if levels:
            over_z(levels - 1, n, d, j)
        else:
            z_carry[d, j] = jnp.zeros((wy, DV), F32)
        spread(d, j, z_carry[d, j], y_in, d_y, ny, y_out)
        send_y(n, d, j)

    def send_y(n, d, j):
        for o in ys:
            go(y_out.at[o, d, j], row_carry.at[d, j, rows_of(y, wy), :], s_yout, r_yout.at[n], y_id(o))
        row_carry[d, j, rows_of(y, wy), :] = y_out[y, d, j]

    def starts(d, at):
        row = jnp.logical_and(z == (0 if d == 0 else nz - 1), y == (0 if d == 0 else ny - 1))
        return jnp.logical_and(row, at == (0 if d == 0 else nx - 1))

    def down_y(n, d, j):
        if ny > 1:
            landed(row_carry.at[d, j, pl.ds(0, (ny - 1) * wy), :], r_yout.at[n])
        spread(d, j, row_carry[d, j], x_in, d_x, nx, x_out)
        for o in xs:
            c = copy(
                x_out.at[o, d, j], carry.at[d, j, rows_of(x, wx), :], s_xout.at[d], r_xout.at[n], x_id(o)
            )
            pl.when(jnp.logical_not(starts(d, o)))(c.start)
        carry[d, j, rows_of(x, wx), :] = x_out[x, d, j]

    def down_x(n, d, j):
        starting = starts(d, x)

        @pl.when(starting)
        def _():
            carry[d, j] = jnp.zeros((DK, DV), F32)

        @pl.when(jnp.logical_not(starting))
        def _():
            landed(carry.at[d, j, pl.ds(0, (nx - 1) * wx), :], r_xout.at[n])

        near = first if d == 0 else jnp.logical_not(first)

        @pl.when(near)
        def _():
            got = carry[d, j]
            back_buf[d, j] = d_core[mine + j] * got + total_buf[d, mine + j]
            from_buf[d, mine + j] = got

        @pl.when(jnp.logical_not(near))
        def _():
            got = carry[d, j]
            back_buf[d, j] = got
            from_buf[d, mine + j] = d_mate[mine + j] * got + peer_buf[d, j]

        go(back_buf.at[d, j], from_buf.at[d, mine + j], s_back, r_back.at[n], mate)
        outer(d, mine + j)

    def finish(n, d, j):
        landed(from_buf.at[d, theirs + j], r_back.at[n])
        outer(d, theirs + j)

    def load_more(k):
        for head in (theirs + k, mine + k):
            load(head, 0, k + 3)
            load(head, 1, k + 3)

    def greet_mate():
        go(d_core, d_mate, s_d, r_d.at[0], mate)
        send_core(0, *chunks[0])

    totals = (forward_total, reverse_total)
    ready(0, 0)
    forward_total(theirs)
    hear(0, 1 + CORES * (nx + ny - 2))
    pl.when(core == 0)(greet_mate)
    ready(0, 2)
    forward_total(mine)
    learn(0)
    pl.when(core != 0)(greet_mate)
    load_more(1)
    ready(0, 1)
    reverse_total(theirs)
    send_core(1, *chunks[1])
    landed(d_mate, r_d.at[0])
    d_x[x] = d_core[...] * d_mate[...]
    for o in xs:
        go(d_x.at[x], d_x.at[x], s_d, r_d.at[1], x_id(o))
    join_cores(0, *chunks[0])
    for k in range(2, half):
        load_more(k)
    ready(0, 3)
    reverse_total(mine)
    join_cores(1, *chunks[1])
    late = []
    for k in range(1, half):
        ready(k, k + 3)
        turn = [n for n, (_, j) in enumerate(chunks) if j == k]
        for n in turn:
            totals[chunks[n][0]](theirs + k)
            send_core(n, *chunks[n])
            for m in late:
                join_cores(m, *chunks[m])
            late = []
        for n in turn:
            totals[chunks[n][0]](mine + k)
        join_cores(turn[0], *chunks[turn[0]])
        late = turn[1:]
    for m in late:
        join_cores(m, *chunks[m])

    def inside(n, d, j):
        for h in range(n, HEAD_COUNT, len(chunks)):
            intra(h)

    climb = [(2 + level, functools.partial(over_z, level)) for level in range(levels - 1)]
    top = 2 + len(climb)
    back = len(chunks)
    stages = [(0, up_x), (0, inside), (top + 2, down_y), (back + 2, finish), (back, down_x)]
    stages += [(1, up_y)] + climb + [(top, down_z)]
    for slot in range(2 * len(chunks) + 2):
        for lag, stage in stages:
            n = slot - lag
            if 0 <= n < len(chunks):
                stage(n, *chunks[n])

    left(peer_buf, s_core)
    left(x_in.at[pl.ds(0, nx - 1)], s_x)
    withheld = [
        sum(jnp.where(starts(d, o), 1, 0) for o in xs) for d in range(2)
    ]
    for d in range(2):
        for amount in (nx - 2, nx - 1):
            if amount:
                pl.when(withheld[d] == nx - 1 - amount)(
                    functools.partial(left, x_out.at[pl.ds(0, amount), d], s_xout.at[d])
                )
    left(back_buf, s_back)
    left(decay_rows.at[pl.ds(0, nx + ny + nz - 2)], s_d)
    if ny > 1:
        left(y_in.at[pl.ds(0, ny - 1)], s_y)
        left(y_out.at[pl.ds(0, ny - 1)], s_yout)
    if nz > 1:
        sends = sum(
            jnp.where(needed, 1, 0)
            for level in range(levels) for d in range(2) for _, needed in z_sends(d, level)
        )
        for amount in range(1, nz):
            pl.when(sends == amount)(functools.partial(left, z_in.at[pl.ds(0, amount)], s_z))


def write_kernel(gq_ref, gk_ref, gv_ref, gq_hbm, gk_hbm, gv_hbm, sems):
    copies = [
        pltpu.make_async_copy(near, far, sems.at[i])
        for i, (near, far) in enumerate(((gq_ref, gq_hbm), (gk_ref, gk_hbm), (gv_ref, gv_hbm)))
    ]
    for c in copies:
        c.start()
    for c in copies:
        c.wait()


def body(nx, ny, nz, queries, keys, values, grad_out, log_decay):
    tokens = queries.shape[0]
    count = tokens // BLOCK
    half = HEAD_COUNT // CORES
    wx = DK // nx
    wy = wx // ny
    levels = (nz - 1).bit_length()
    n = 2 * half
    vm = pl.BlockSpec(memory_space=pltpu.VMEM)
    hbm = pl.BlockSpec(memory_space=pltpu.HBM)
    dma = pltpu.SemaphoreType.DMA

    def states(*lead):
        return pltpu.VMEM(lead + (DV,), F32)

    def decays(*lead):
        return pltpu.VMEM(lead + (HEAD_COUNT, 1, DV), F32)

    out = jax.ShapeDtypeStruct((tokens, HEAD_COUNT * DK), BF16)
    near = pltpu.VMEM(out.shape, out.dtype)
    grads = pl.pallas_call(
        functools.partial(retention_kernel, nx, ny, nz),
        out_shape=(near, near, near),
        in_specs=[hbm] * 5,
        out_specs=(vm, vm, vm),
        scratch_shapes=[
            pltpu.VMEM((HEAD_COUNT, tokens), F32),
            pltpu.VMEM((4, tokens, HEAD_COUNT * DK), BF16),
            pltpu.VMEM((count, HEAD_COUNT, 1, BLOCK), F32),
            states(2, max(1, count - 1), HEAD_COUNT, DK),
            states(3, HEAD_COUNT, tokens),
            states(2, HEAD_COUNT, DK), states(2, HEAD_COUNT, DK),
            states(2, half, DK), states(2, half, DK),
            states(2, half, DK), states(nx, 2, half, wx), states(2, half, wx),
            states(ny, 2, half, wy), states(2, half, wy),
            states(max(2 * levels, nz), half, wy), states(max(1, levels - 1), 2, half, wy), states(2, half, wy),
            states(ny, 2, half, wy), states(2, half, wx),
            states(nx, 2, half, wx), states(2, half, DK),
            decays(2 + nx + ny + nz), decays(max(1, levels), 2), pltpu.SemaphoreType.REGULAR, dma, dma((half + 3,)),
            dma, dma((n,)), dma((nx,)), dma, dma((n,)), dma, dma((n,)), dma, dma((max(1, levels), n)),
            dma, dma((n,)), dma((2,)), dma((n,)), dma, dma((n,)), dma, dma((4,)),
        ],
        compiler_params=pltpu.CompilerParams(collective_id=0, has_side_effects=True, vmem_limit_bytes=52 << 20),
        name="retention",
    )(pltpu.with_memory_space_constraint(log_decay, pltpu.HBM), queries, keys, values, grad_out)
    return pl.pallas_call(
        write_kernel,
        out_shape=(out, out, out),
        in_specs=[vm] * 3,
        out_specs=(hbm, hbm, hbm),
        scratch_shapes=[dma((3,))],
        name="write",
    )(*(pltpu.with_memory_space_constraint(g, pltpu.VMEM) for g in grads))


def solution(mesh):
    nx = mesh.shape["mem"] // CORES
    ny = nx if mesh.shape["grp"] % nx == 0 else 1
    nz = mesh.shape["grp"] // ny
    tokens = P(("grp", "mem"), None)
    return jax.shard_map(
        functools.partial(body, nx, ny, nz),
        mesh=mesh,
        in_specs=(tokens, tokens, tokens, tokens, P(None, ("grp", "mem"))),
        out_specs=(tokens, tokens, tokens),
        check_vma=False,
    )
```

```python
import functools

import jax
import jax.numpy as jnp
from jax import lax
from jax.experimental import pallas as pl
from jax.experimental.pallas import tpu as pltpu
from jax.sharding import PartitionSpec as P

HEAD_COUNT = 8
DK = 256
DV = 256
BLOCK = 128
CORES = 2
KEYS, VALUES, QUERIES, GRADS = range(4)
MESH = pl.DeviceIdType.MESH
F32 = jnp.float32
BF16 = jnp.bfloat16


def dot(a, b, ca, cb):
    return lax.dot_general(a, b, (((ca,), (cb,)), ((), ())), preferred_element_type=F32)


def spread_rows(row):
    flat = jnp.broadcast_to(row, (BLOCK, BLOCK))
    return flat, flat.T


def wide(mat, width):
    return jnp.concatenate([mat] * (width // BLOCK), axis=1)


def retention_kernel(
    nx, ny, nz, logs_hbm, q_hbm, k_hbm, v_hbm, g_hbm, gq_ref, gk_ref, gv_ref,
    logs_ref, toks, cum, local, inner, total_buf, from_buf, peer_buf, back_buf,
    chip_buf, x_in, row_tot, y_in, plane_tot, z_in, z_out, z_carry, y_out, row_carry, x_out, carry,
    decay_rows, weights, s_meet, s_logs, s_in, s_core, r_core, r_first, s_x, r_x, s_y, r_y, s_z, r_z,
    s_yout, r_yout, s_xout, r_xout, s_back, r_back, s_d, r_d,
):
    count = logs_ref.shape[1] // BLOCK
    scale = DK ** (-0.5)
    half = HEAD_COUNT // CORES
    wx = DK // nx
    wy = wx // ny
    d_core, d_mate = decay_rows.at[0], decay_rows.at[1]
    d_x, d_y = decay_rows.at[pl.ds(2, nx)], decay_rows.at[pl.ds(2 + nx, ny)]
    d_z = decay_rows.at[pl.ds(2 + nx + ny, nz)]
    early = max(1, half - 2)
    chunks = [(d, k) for k in range(early) for d in range(2)]
    chunks += [(d, k) for d in (1, 0) for k in range(early, half)]
    grp, mem = lax.axis_index("grp"), lax.axis_index("mem")
    z, y = grp // ny, lax.rem(grp, ny)
    x, core = mem // CORES, lax.rem(mem, CORES)
    mate = (grp, x * CORES + 1 - core)

    def x_id(to):
        return (grp, to * CORES + core)

    def y_id(to):
        return (z * ny + to, mem)

    def z_id(to):
        return (to * ny + y, mem)

    xs = [lax.rem(x + off, nx) for off in range(1, nx)]
    ys = [lax.rem(y + off, ny) for off in range(1, ny)]
    zs = [lax.rem(z + off, nz) for off in range(1, nz)]
    barrier = pltpu.get_barrier_semaphore()

    def tell(sem, device):
        pl.semaphore_signal(sem, inc=1, device_id=device, device_id_type=MESH)

    for device in [(grp, o * CORES) for o in xs] + [(z * ny + o, x * CORES) for o in ys]:
        tell(barrier, device)
    pl.when(core == 1)(lambda: tell(barrier, mate))
    for o in zs:
        tell(barrier, (o * ny + y, x * CORES + 1))

    def hear(hearer, signals):
        @pl.when(core == hearer)
        def _():
            pl.semaphore_wait(barrier, signals)
            tell(s_meet, mate)

    def learn(hearer):
        @pl.when(core != hearer)
        def _():
            pl.semaphore_wait(s_meet, 1)

    def copy(src, dst, send, recv, device):
        return pltpu.make_async_remote_copy(
            src_ref=src, dst_ref=dst, send_sem=send, recv_sem=recv,
            device_id=device, device_id_type=MESH,
        )

    def go(*args):
        copy(*args).start()

    def landed(ref, sem):
        copy(ref, ref, s_back, sem, mate).wait_recv()

    def left(ref, sem):
        copy(ref, ref, sem, r_back.at[0], mate).wait_send()

    def members(d, size):
        return range(size) if d == 0 else range(size - 1, -1, -1)

    mine, theirs = core * half, (1 - core) * half

    def rows_of(c, size):
        return pl.ds(pl.multiple_of(c * size, size), size)

    def cols_of(head, size):
        return pl.ds(pl.multiple_of(head * size, size), size)

    def tokens_of(b):
        return pl.ds(b * BLOCK, BLOCK)

    load_logs = pltpu.make_async_copy(logs_hbm, logs_ref, s_logs)
    load_logs.start()

    def load(head, pair, slot):
        part = cols_of(head, DK)
        for i in (2 * pair, 2 * pair + 1):
            far = (k_hbm, v_hbm, q_hbm, g_hbm)[i]
            pltpu.make_async_copy(far.at[:, part], toks.at[i, :, part], s_in.at[slot]).start()

    load(theirs, 0, 0)
    load(mine, 0, 2)

    def ready(k, slot):
        held = toks.at[:, :, pl.ds(0, CORES * DK)] if k else toks.at[pl.ds(0, 2), :, pl.ds(0, DK)]
        pltpu.make_async_copy(held, held, s_in.at[slot]).wait()

    def tok(i, head, b):
        return toks[i, tokens_of(b), cols_of(head, DK)]

    square = (BLOCK, BLOCK)
    lower = lax.broadcasted_iota(jnp.int32, square, 0) >= lax.broadcasted_iota(jnp.int32, square, 1)
    ones = jnp.where(lower, 1.0, 0.0)
    load_logs.wait()
    load(theirs, 1, 1)
    load(mine, 1, 3)
    carried = None
    for b in range(count):
        row = lax.dot_general(
            logs_ref[:, b * BLOCK:(b + 1) * BLOCK], ones, (((1,), (1,)), ((), ())),
            precision=lax.Precision.HIGHEST, preferred_element_type=F32,
        )
        for h in range(HEAD_COUNT):
            cum[b, h] = row[h:h + 1, :]
        whole = jnp.exp(row[:, BLOCK - 1:BLOCK])
        carried = whole if carried is None else carried * whole
    carried = jnp.broadcast_to(carried, (HEAD_COUNT, DV))
    for h in range(HEAD_COUNT):
        d_core[h] = carried[h:h + 1, :]
    def factors(head, b):
        row = cum[b, head]
        flat, cols = spread_rows(row)
        end = row[:, BLOCK - 1:BLOCK]
        return flat, cols, end

    def forward_total(head):
        forward = None
        for b in range(count):
            _, cols, end = factors(head, b)
            kd = tok(KEYS, head, b).astype(F32) * wide(jnp.exp(end - cols), DK)
            whole = jnp.broadcast_to(jnp.exp(end), (1, DV))
            part = dot(kd.astype(BF16), tok(VALUES, head, b), 0, 0)
            if b > 0:
                local[0, b - 1, head] = forward
            forward = part if forward is None else whole * forward + part
        total_buf[0, head] = forward

    def reverse_total(head):
        back = None
        for b in reversed(range(count)):
            _, cols, end = factors(head, b)
            qd = tok(QUERIES, head, b).astype(F32) * wide(jnp.exp(cols), DK)
            whole = jnp.broadcast_to(jnp.exp(end), (1, DV))
            part = dot(qd.astype(BF16), tok(GRADS, head, b), 0, 0)
            if b < count - 1:
                local[1, b, head] = back
            back = part if back is None else whole * back + part
        total_buf[1, head] = back

    def intra(head):
        for b in range(count):
            flat, cols, _ = factors(head, b)
            decay = jnp.where(lower, jnp.exp(jnp.where(lower, cols - flat, 0.0)), 0.0)
            q, k = tok(QUERIES, head, b), tok(KEYS, head, b)
            v, g = tok(VALUES, head, b), tok(GRADS, head, b)
            wg = (dot(g, v, 1, 1) * decay).astype(BF16)
            wv = (dot(q, k, 1, 1) * decay).astype(BF16)
            inner[0, head, tokens_of(b), :] = dot(wg, k, 1, 0)
            inner[1, head, tokens_of(b), :] = dot(wg, q, 0, 0)
            inner[2, head, tokens_of(b), :] = dot(wv, g, 0, 0)

    def outer(d, head):
        coming = from_buf[d, head]
        weight = None
        for step, b in enumerate(members(d, count)):
            _, cols, end = factors(head, b)
            if step == 0:
                low = coming.astype(BF16)
            else:
                low = (local[d, b - 1 if d == 0 else b, head] + weight * coming).astype(BF16)
            whole = jnp.broadcast_to(jnp.exp(end), (1, DV))
            weight = whole if weight is None else weight * whole
            if d == 0:
                far = wide(jnp.exp(cols), DK) * dot(tok(GRADS, head, b), low, 1, 1)
                near = inner[0, head, tokens_of(b), :]
                gq_ref[tokens_of(b), cols_of(head, DK)] = (scale * (near + far)).astype(BF16)
            else:
                tail = wide(jnp.exp(end - cols), DK)
                near = inner[1, head, tokens_of(b), :]
                far = tail * dot(tok(VALUES, head, b), low, 1, 1)
                gk_ref[tokens_of(b), cols_of(head, DK)] = (scale * (near + far)).astype(BF16)
                near = inner[2, head, tokens_of(b), :]
                far = tail * dot(tok(KEYS, head, b), low, 1, 0)
                gv_ref[tokens_of(b), cols_of(head, DV)] = (scale * (near + far)).astype(BF16)

    first = core == 0

    def send_core(n, d, j):
        if n:
            go(total_buf.at[d, theirs + j], peer_buf.at[d, j], s_core, r_core.at[n], mate)
        else:
            for i, o in enumerate(xs + [x]):
                part = rows_of(o, wx)
                go(total_buf.at[d, theirs + j, part, :], peer_buf.at[d, j, part, :],
                   s_core, r_first.at[i], mate)

    def join_cores(n, d, j):
        if n:
            landed(peer_buf.at[d, j], r_core.at[n])
        own_d, peer_d = d_core[mine + j], d_mate[mine + j]
        one = jnp.ones_like(own_d)
        if d == 0:
            w_own, w_peer = jnp.where(first, peer_d, one), jnp.where(first, one, own_d)
        else:
            w_own, w_peer = jnp.where(first, one, peer_d), jnp.where(first, own_d, one)

        def joined(o):
            part = rows_of(o, wx)
            return w_own * total_buf[d, mine + j, part, :] + w_peer * peer_buf[d, j, part, :]

        for i, o in enumerate(xs):
            if n == 0:
                landed(peer_buf.at[d, j, rows_of(o, wx), :], r_first.at[i])
            chip_buf[d, j, rows_of(o, wx), :] = joined(o)
            go(chip_buf.at[d, j, rows_of(o, wx), :], x_in.at[x, d, j], s_x, r_x.at[n], x_id(o))
        if n == 0:
            landed(peer_buf.at[d, j, rows_of(x, wx), :], r_first.at[nx - 1])
        x_in[x, d, j] = joined(x)

    def fold(d, j, parts, decays, size):
        running = None
        for c in members(d, size):
            part = parts[c, d, j]
            running = part if running is None else decays[c, mine + j] * running + part
        return running

    def up_x(n, d, j):
        if n == 0:
            landed(d_x.at[pl.ds(0, nx - 1)], r_d.at[1])
            product = d_x[0]
            for c in range(1, nx):
                product = product * d_x[c]
            d_y[y] = product
            for o in ys:
                go(d_y.at[y], d_y.at[y], s_d, r_d.at[2], y_id(o))
        landed(x_in.at[pl.ds(0, nx - 1), d, j], r_x.at[n])
        row_tot[d, j] = fold(d, j, x_in, d_x, nx)
        for o in ys:
            go(row_tot.at[d, j, rows_of(o, wy), :], y_in.at[y, d, j], s_y, r_y.at[n], y_id(o))
        y_in[y, d, j] = row_tot[d, j, rows_of(y, wy), :]

    def up_y(n, d, j):
        if n == 0:
            if ny > 1:
                landed(d_y.at[pl.ds(0, ny - 1)], r_d.at[2])
            product = d_y[0]
            for c in range(1, ny):
                product = product * d_y[c]
            d_z[z] = product
            if nz > 1:
                hear(1, CORES * (nz - 1))
                learn(1)
            for t in zs:
                go(d_z.at[z], d_z.at[z], s_d, r_d.at[3], z_id(t))
        if ny > 1:
            landed(y_in.at[pl.ds(0, ny - 1), d, j], r_y.at[n])
        plane_tot[d, j] = fold(d, j, y_in, d_y, ny)
        send_z(n, d, j, 0, plane_tot.at[d, j])

    levels = (nz - 1).bit_length()

    def place(d):
        return z if d == 0 else nz - 1 - z

    def z_sends(d, level):
        size, p = 1 << level, place(d)
        last = lax.rem(p, 2 * size) == size - 1
        return [(i + 1, jnp.logical_and(last, p + i + 1 < nz)) for i in range(size)]

    def z_hears(d, level):
        return lax.rem(place(d), 2 << level) >= 1 << level

    def send_z(n, d, j, level, src):
        if level < levels:
            for hop, needed in z_sends(d, level):
                to = lax.rem(z + hop, nz) if d == 0 else lax.rem(z - hop + nz, nz)
                c = copy(src, z_in.at[2 * level + d, j], s_z, r_z.at[level, n], z_id(to))
                pl.when(needed)(c.start)

    def z_weight(d, level):
        size = 1 << level
        start = place(d) // size * size
        weight = jnp.ones_like(d_core[...])
        for i in range(size - 1):
            q = lax.rem(start + i, nz)
            passed = d_z[q if d == 0 else nz - 1 - q]
            weight = jnp.where(start + i < place(d), weight * passed, weight)
        return weight

    def spread(d, j, held, parts, decays, size, out):
        last = members(d, size)[-1]
        for c in members(d, size):
            out[c, d, j] = held
            if c != last:
                held = decays[c, mine + j] * held + parts[c, d, j]

    def over_z(level, n, d, j):
        if n == 0 and level == 0:
            landed(d_z.at[pl.ds(0, nz - 1)], r_d.at[3])
            for side in range(2):
                for upper in range(levels):
                    weights[upper, side] = z_weight(side, upper)
        if level == 0:
            z_carry[d, j] = jnp.zeros((wy, DV), F32)

        @pl.when(z_hears(d, level))
        def _():
            landed(z_in.at[2 * level + d, j], r_z.at[level, n])
            came = z_in[2 * level + d, j]
            if level:
                came = weights[level, d, mine + j] * came + z_carry[d, j]
            z_carry[d, j] = came

        if level + 1 < levels:
            @pl.when(z_sends(d, level + 1)[0][1])
            def _():
                z_out[level, d, j] = d_z[z, mine + j] * z_carry[d, j] + plane_tot[d, j]

            send_z(n, d, j, level + 1, z_out.at[level, d, j])

    def down_z(n, d, j):
        if levels:
            over_z(levels - 1, n, d, j)
        else:
            z_carry[d, j] = jnp.zeros((wy, DV), F32)
        spread(d, j, z_carry[d, j], y_in, d_y, ny, y_out)
        send_y(n, d, j)

    def send_y(n, d, j):
        for o in ys:
            go(y_out.at[o, d, j], row_carry.at[d, j, rows_of(y, wy), :], s_yout, r_yout.at[n], y_id(o))
        row_carry[d, j, rows_of(y, wy), :] = y_out[y, d, j]

    def starts(d, at):
        row = jnp.logical_and(z == (0 if d == 0 else nz - 1), y == (0 if d == 0 else ny - 1))
        return jnp.logical_and(row, at == (0 if d == 0 else nx - 1))

    def send_x(n, d, j, ready=True):
        for o in xs:
            c = copy(
                x_out.at[o, d, j], carry.at[d, j, rows_of(x, wx), :], s_xout.at[d], r_xout.at[n], x_id(o)
            )
            pl.when(jnp.logical_and(jnp.logical_not(starts(d, o)), ready))(c.start)

    final = len(chunks) - 1

    def down_y(n, d, j):
        if ny > 1:
            landed(row_carry.at[d, j, pl.ds(0, (ny - 1) * wy), :], r_yout.at[n])
        spread(d, j, row_carry[d, j], x_in, d_x, nx, x_out)
        send_x(n, d, j, core == 0 if n == final else True)
        carry[d, j, rows_of(x, wx), :] = x_out[x, d, j]

    def down_x(n, d, j):
        starting = starts(d, x)

        @pl.when(starting)
        def _():
            carry[d, j] = jnp.zeros((DK, DV), F32)

        @pl.when(jnp.logical_not(starting))
        def _():
            landed(carry.at[d, j, pl.ds(0, (nx - 1) * wx), :], r_xout.at[n])

        if n == final - 1:
            send_x(final, *chunks[final], core != 0)
        near = first if d == 0 else jnp.logical_not(first)

        @pl.when(near)
        def _():
            got = carry[d, j]
            back_buf[d, j] = d_core[mine + j] * got + total_buf[d, mine + j]
            from_buf[d, mine + j] = got

        @pl.when(jnp.logical_not(near))
        def _():
            got = carry[d, j]
            back_buf[d, j] = got
            from_buf[d, mine + j] = d_mate[mine + j] * got + peer_buf[d, j]

        go(back_buf.at[d, j], from_buf.at[d, mine + j], s_back, r_back.at[n], mate)
        outer(d, mine + j)

    def finish(n, d, j):
        landed(from_buf.at[d, theirs + j], r_back.at[n])
        outer(d, theirs + j)

    def load_more(k):
        for head in (theirs + k, mine + k):
            load(head, 0, k + 3)
            load(head, 1, k + 3)

    def greet_mate():
        go(d_core, d_mate, s_d, r_d.at[0], mate)
        send_core(0, *chunks[0])

    totals = (forward_total, reverse_total)
    ready(0, 0)
    forward_total(theirs)
    hear(0, 1 + CORES * (nx + ny - 2))
    pl.when(core == 0)(greet_mate)
    ready(0, 2)
    forward_total(mine)
    learn(0)
    pl.when(core != 0)(greet_mate)
    load_more(1)
    ready(0, 1)
    reverse_total(theirs)
    send_core(1, *chunks[1])
    landed(d_mate, r_d.at[0])
    d_x[x] = d_core[...] * d_mate[...]
    for o in xs:
        go(d_x.at[x], d_x.at[x], s_d, r_d.at[1], x_id(o))
    join_cores(0, *chunks[0])
    for k in range(2, half):
        load_more(k)
    ready(0, 3)
    reverse_total(mine)
    join_cores(1, *chunks[1])
    late, held = [], {0}
    for turn in (range(n, n + 2) for n in range(2, len(chunks), 2)):
        for n in turn:
            d, k = chunks[n]
            if k not in held:
                ready(k, k + 3)
                held.add(k)
            totals[d](theirs + k)
            send_core(n, d, k)
            for m in late:
                join_cores(m, *chunks[m])
            late = []
        for n in turn:
            totals[chunks[n][0]](mine + chunks[n][1])
        join_cores(turn[0], *chunks[turn[0]])
        late = turn[1:]
    for m in late:
        join_cores(m, *chunks[m])

    def inside(n, d, j):
        for h in range(n, HEAD_COUNT, len(chunks)):
            intra(h)

    climb = [(2 + level, functools.partial(over_z, level)) for level in range(levels - 1)]
    top = 2 + len(climb)
    back = len(chunks)
    stages = [(0, up_x), (0, inside), (top + 2, down_y), (back + 2, finish), (back, down_x)]
    stages += [(1, up_y)] + climb + [(top, down_z)]
    for slot in range(2 * len(chunks) + 1):
        for lag, stage in stages:
            n = slot - lag
            if stage is finish and n >= final - 1:
                n = final
            if 0 <= n < len(chunks):
                stage(n, *chunks[n])
            if stage is finish and n == final - 2:
                finish(final - 1, *chunks[final - 1])

    left(peer_buf, s_core)
    left(x_in.at[pl.ds(0, nx - 1)], s_x)
    withheld = [
        sum(jnp.where(starts(d, o), 1, 0) for o in xs) for d in range(2)
    ]
    for d in range(2):
        for amount in (nx - 2, nx - 1):
            if amount:
                pl.when(withheld[d] == nx - 1 - amount)(
                    functools.partial(left, x_out.at[pl.ds(0, amount), d], s_xout.at[d])
                )
    left(back_buf, s_back)
    left(decay_rows.at[pl.ds(0, nx + ny + nz - 2)], s_d)
    if ny > 1:
        left(y_in.at[pl.ds(0, ny - 1)], s_y)
        left(y_out.at[pl.ds(0, ny - 1)], s_yout)
    if nz > 1:
        sends = sum(
            jnp.where(needed, 1, 0)
            for level in range(levels) for d in range(2) for _, needed in z_sends(d, level)
        )
        for amount in range(1, nz):
            pl.when(sends == amount)(functools.partial(left, z_in.at[pl.ds(0, amount)], s_z))


def write_kernel(gq_ref, gk_ref, gv_ref, gq_hbm, gk_hbm, gv_hbm, sems):
    copies = [
        pltpu.make_async_copy(near, far, sems.at[i])
        for i, (near, far) in enumerate(((gq_ref, gq_hbm), (gk_ref, gk_hbm), (gv_ref, gv_hbm)))
    ]
    for c in copies:
        c.start()
    for c in copies:
        c.wait()


def body(nx, ny, nz, queries, keys, values, grad_out, log_decay):
    tokens = queries.shape[0]
    count = tokens // BLOCK
    half = HEAD_COUNT // CORES
    wx = DK // nx
    wy = wx // ny
    levels = (nz - 1).bit_length()
    n = 2 * half
    vm = pl.BlockSpec(memory_space=pltpu.VMEM)
    hbm = pl.BlockSpec(memory_space=pltpu.HBM)
    dma = pltpu.SemaphoreType.DMA

    def states(*lead):
        return pltpu.VMEM(lead + (DV,), F32)

    def decays(*lead):
        return pltpu.VMEM(lead + (HEAD_COUNT, 1, DV), F32)

    out = jax.ShapeDtypeStruct((tokens, HEAD_COUNT * DK), BF16)
    near = pltpu.VMEM(out.shape, out.dtype)
    grads = pl.pallas_call(
        functools.partial(retention_kernel, nx, ny, nz),
        out_shape=(near, near, near),
        in_specs=[hbm] * 5,
        out_specs=(vm, vm, vm),
        scratch_shapes=[
            pltpu.VMEM((HEAD_COUNT, tokens), F32),
            pltpu.VMEM((4, tokens, HEAD_COUNT * DK), BF16),
            pltpu.VMEM((count, HEAD_COUNT, 1, BLOCK), F32),
            states(2, max(1, count - 1), HEAD_COUNT, DK),
            states(3, HEAD_COUNT, tokens),
            states(2, HEAD_COUNT, DK), states(2, HEAD_COUNT, DK),
            states(2, half, DK), states(2, half, DK),
            states(2, half, DK), states(nx, 2, half, wx), states(2, half, wx),
            states(ny, 2, half, wy), states(2, half, wy),
            states(max(2 * levels, nz), half, wy), states(max(1, levels - 1), 2, half, wy), states(2, half, wy),
            states(ny, 2, half, wy), states(2, half, wx),
            states(nx, 2, half, wx), states(2, half, DK),
            decays(2 + nx + ny + nz), decays(max(1, levels), 2), pltpu.SemaphoreType.REGULAR, dma, dma((half + 3,)),
            dma, dma((n,)), dma((nx,)), dma, dma((n,)), dma, dma((n,)), dma, dma((max(1, levels), n)),
            dma, dma((n,)), dma((2,)), dma((n,)), dma, dma((n,)), dma, dma((4,)),
        ],
        compiler_params=pltpu.CompilerParams(collective_id=0, has_side_effects=True, vmem_limit_bytes=52 << 20),
        name="retention",
    )(pltpu.with_memory_space_constraint(log_decay, pltpu.HBM), queries, keys, values, grad_out)
    return pl.pallas_call(
        write_kernel,
        out_shape=(out, out, out),
        in_specs=[vm] * 3,
        out_specs=(hbm, hbm, hbm),
        scratch_shapes=[dma((3,))],
        name="write",
    )(*(pltpu.with_memory_space_constraint(g, pltpu.VMEM) for g in grads))


def solution(mesh):
    nx = mesh.shape["mem"] // CORES
    ny = nx if mesh.shape["grp"] % nx == 0 else 1
    nz = mesh.shape["grp"] // ny
    tokens = P(("grp", "mem"), None)
    return jax.shard_map(
        functools.partial(body, nx, ny, nz),
        mesh=mesh,
        in_specs=(tokens, tokens, tokens, tokens, P(None, ("grp", "mem"))),
        out_specs=(tokens, tokens, tokens),
        check_vma=False,
    )
```

```python
import functools

import jax
import jax.numpy as jnp
from jax import lax
from jax.experimental import pallas as pl
from jax.experimental.pallas import tpu as pltpu
from jax.sharding import PartitionSpec as P

HEAD_COUNT = 8
DK = 256
DV = 256
BLOCK = 128
CORES = 2
KEYS, VALUES, QUERIES, GRADS = range(4)
MESH = pl.DeviceIdType.MESH
F32 = jnp.float32
BF16 = jnp.bfloat16


def dot(a, b, ca, cb):
    return lax.dot_general(a, b, (((ca,), (cb,)), ((), ())), preferred_element_type=F32)


def spread_rows(row):
    flat = jnp.broadcast_to(row, (BLOCK, BLOCK))
    return flat, flat.T


def wide(mat, width):
    return jnp.concatenate([mat] * (width // BLOCK), axis=1)


def retention_kernel(
    nx, ny, nz, logs_hbm, q_hbm, k_hbm, v_hbm, g_hbm, gq_ref, gk_ref, gv_ref,
    logs_ref, toks, cum, local, inner, total_buf, from_buf, peer_buf, back_buf,
    chip_buf, x_in, row_tot, y_in, plane_tot, z_in, z_out, z_carry, y_out, row_carry, x_out, carry,
    decay_rows, weights, s_meet, s_logs, s_in, s_core, r_core, r_first, s_x, r_x, s_y, r_y, s_z, r_z,
    s_yout, r_yout, s_xout, r_xout, r_tail, s_back, r_back, s_d, r_d,
):
    count = logs_ref.shape[1] // BLOCK
    scale = DK ** (-0.5)
    half = HEAD_COUNT // CORES
    wx = DK // nx
    wy = wx // ny
    d_core, d_mate = decay_rows.at[0], decay_rows.at[1]
    d_x, d_y = decay_rows.at[pl.ds(2, nx)], decay_rows.at[pl.ds(2 + nx, ny)]
    d_z = decay_rows.at[pl.ds(2 + nx + ny, nz)]
    early = max(1, half - 2)
    chunks = [(d, k) for k in range(early) for d in range(2)]
    chunks += [(d, k) for d in (1, 0) for k in range(early, half)]
    grp, mem = lax.axis_index("grp"), lax.axis_index("mem")
    z, y = grp // ny, lax.rem(grp, ny)
    x, core = mem // CORES, lax.rem(mem, CORES)
    mate = (grp, x * CORES + 1 - core)

    def x_id(to):
        return (grp, to * CORES + core)

    def y_id(to):
        return (z * ny + to, mem)

    def z_id(to):
        return (to * ny + y, mem)

    xs = [lax.rem(x + off, nx) for off in range(1, nx)]
    ys = [lax.rem(y + off, ny) for off in range(1, ny)]
    zs = [lax.rem(z + off, nz) for off in range(1, nz)]
    barrier = pltpu.get_barrier_semaphore()

    def tell(sem, device):
        pl.semaphore_signal(sem, inc=1, device_id=device, device_id_type=MESH)

    for device in [(grp, o * CORES) for o in xs] + [(z * ny + o, x * CORES) for o in ys]:
        tell(barrier, device)
    pl.when(core == 1)(lambda: tell(barrier, mate))
    for o in zs:
        tell(barrier, (o * ny + y, x * CORES + 1))

    def hear(hearer, signals):
        @pl.when(core == hearer)
        def _():
            pl.semaphore_wait(barrier, signals)
            tell(s_meet, mate)

    def learn(hearer):
        @pl.when(core != hearer)
        def _():
            pl.semaphore_wait(s_meet, 1)

    def copy(src, dst, send, recv, device):
        return pltpu.make_async_remote_copy(
            src_ref=src, dst_ref=dst, send_sem=send, recv_sem=recv,
            device_id=device, device_id_type=MESH,
        )

    def go(*args):
        copy(*args).start()

    def landed(ref, sem):
        copy(ref, ref, s_back, sem, mate).wait_recv()

    def left(ref, sem):
        copy(ref, ref, sem, r_back.at[0], mate).wait_send()

    def members(d, size):
        return range(size) if d == 0 else range(size - 1, -1, -1)

    mine, theirs = core * half, (1 - core) * half

    def rows_of(c, size):
        return pl.ds(pl.multiple_of(c * size, size), size)

    def cols_of(head, size):
        return pl.ds(pl.multiple_of(head * size, size), size)

    def tokens_of(b):
        return pl.ds(b * BLOCK, BLOCK)

    load_logs = pltpu.make_async_copy(logs_hbm, logs_ref, s_logs)
    load_logs.start()

    def load(head, pair, slot):
        part = cols_of(head, DK)
        for i in (2 * pair, 2 * pair + 1):
            far = (k_hbm, v_hbm, q_hbm, g_hbm)[i]
            pltpu.make_async_copy(far.at[:, part], toks.at[i, :, part], s_in.at[slot]).start()

    load(theirs, 0, 0)

    def ready(slot, parts, heads):
        held = toks.at[pl.ds(0, parts), :, pl.ds(0, heads * DK)]
        pltpu.make_async_copy(held, held, s_in.at[slot]).wait()

    def tok(i, head, b):
        return toks[i, tokens_of(b), cols_of(head, DK)]

    square = (BLOCK, BLOCK)
    lower = lax.broadcasted_iota(jnp.int32, square, 0) >= lax.broadcasted_iota(jnp.int32, square, 1)
    ones = jnp.where(lower, 1.0, 0.0)
    load_logs.wait()
    load(mine, 0, 2)
    load(theirs, 1, 1)
    load(mine, 1, 1)
    carried = None
    for b in range(count):
        row = lax.dot_general(
            logs_ref[:, b * BLOCK:(b + 1) * BLOCK], ones, (((1,), (1,)), ((), ())),
            precision=lax.Precision.HIGHEST, preferred_element_type=F32,
        )
        for h in range(HEAD_COUNT):
            cum[b, h] = row[h:h + 1, :]
        whole = jnp.exp(row[:, BLOCK - 1:BLOCK])
        carried = whole if carried is None else carried * whole
    carried = jnp.broadcast_to(carried, (HEAD_COUNT, DV))
    for h in range(HEAD_COUNT):
        d_core[h] = carried[h:h + 1, :]
    def factors(head, b):
        row = cum[b, head]
        flat, cols = spread_rows(row)
        end = row[:, BLOCK - 1:BLOCK]
        return flat, cols, end

    def forward_total(head):
        forward = None
        for b in range(count):
            _, cols, end = factors(head, b)
            kd = tok(KEYS, head, b).astype(F32) * wide(jnp.exp(end - cols), DK)
            whole = jnp.broadcast_to(jnp.exp(end), (1, DV))
            part = dot(kd.astype(BF16), tok(VALUES, head, b), 0, 0)
            if b > 0:
                local[0, b - 1, head] = forward
            forward = part if forward is None else whole * forward + part
        total_buf[0, head] = forward

    def reverse_total(head):
        back = None
        for b in reversed(range(count)):
            _, cols, end = factors(head, b)
            qd = tok(QUERIES, head, b).astype(F32) * wide(jnp.exp(cols), DK)
            whole = jnp.broadcast_to(jnp.exp(end), (1, DV))
            part = dot(qd.astype(BF16), tok(GRADS, head, b), 0, 0)
            if b < count - 1:
                local[1, b, head] = back
            back = part if back is None else whole * back + part
        total_buf[1, head] = back

    def intra(head):
        for b in range(count):
            flat, cols, _ = factors(head, b)
            decay = jnp.where(lower, jnp.exp(jnp.where(lower, cols - flat, 0.0)), 0.0)
            q, k = tok(QUERIES, head, b), tok(KEYS, head, b)
            v, g = tok(VALUES, head, b), tok(GRADS, head, b)
            wg = (dot(g, v, 1, 1) * decay).astype(BF16)
            wv = (dot(q, k, 1, 1) * decay).astype(BF16)
            inner[0, head, tokens_of(b), :] = dot(wg, k, 1, 0)
            inner[1, head, tokens_of(b), :] = dot(wg, q, 0, 0)
            inner[2, head, tokens_of(b), :] = dot(wv, g, 0, 0)

    def outer(d, head):
        coming = from_buf[d, head]
        weight = None
        for step, b in enumerate(members(d, count)):
            _, cols, end = factors(head, b)
            if step == 0:
                low = coming.astype(BF16)
            else:
                low = (local[d, b - 1 if d == 0 else b, head] + weight * coming).astype(BF16)
            whole = jnp.broadcast_to(jnp.exp(end), (1, DV))
            weight = whole if weight is None else weight * whole
            if d == 0:
                far = wide(jnp.exp(cols), DK) * dot(tok(GRADS, head, b), low, 1, 1)
                near = inner[0, head, tokens_of(b), :]
                gq_ref[tokens_of(b), cols_of(head, DK)] = (scale * (near + far)).astype(BF16)
            else:
                tail = wide(jnp.exp(end - cols), DK)
                near = inner[1, head, tokens_of(b), :]
                far = tail * dot(tok(VALUES, head, b), low, 1, 1)
                gk_ref[tokens_of(b), cols_of(head, DK)] = (scale * (near + far)).astype(BF16)
                near = inner[2, head, tokens_of(b), :]
                far = tail * dot(tok(KEYS, head, b), low, 1, 0)
                gv_ref[tokens_of(b), cols_of(head, DV)] = (scale * (near + far)).astype(BF16)

    first = core == 0

    def send_core(n, d, j):
        if n:
            go(total_buf.at[d, theirs + j], peer_buf.at[d, j], s_core, r_core.at[n // 2], mate)
        else:
            for i, o in enumerate(xs + [x]):
                part = rows_of(o, wx)
                go(total_buf.at[d, theirs + j, part, :], peer_buf.at[d, j, part, :],
                   s_core, r_first.at[i], mate)

    def join_cores(n, d, j):
        if n == 1:
            landed(peer_buf.at[d, j], r_core.at[0])
        elif n and n % 2 == 0:
            landed(peer_buf.at[0, pl.ds(0, 2)], r_core.at[n // 2])
        own_d, peer_d = d_core[mine + j], d_mate[mine + j]
        one = jnp.ones_like(own_d)
        if d == 0:
            w_own, w_peer = jnp.where(first, peer_d, one), jnp.where(first, one, own_d)
        else:
            w_own, w_peer = jnp.where(first, one, peer_d), jnp.where(first, own_d, one)

        def joined(o):
            part = rows_of(o, wx)
            return w_own * total_buf[d, mine + j, part, :] + w_peer * peer_buf[d, j, part, :]

        for i, o in enumerate(xs):
            if n == 0:
                landed(peer_buf.at[d, j, rows_of(o, wx), :], r_first.at[i])
            chip_buf[d, j, rows_of(o, wx), :] = joined(o)
            go(chip_buf.at[d, j, rows_of(o, wx), :], x_in.at[x, d, j], s_x, r_x.at[n], x_id(o))
        if n == 0:
            landed(peer_buf.at[d, j, rows_of(x, wx), :], r_first.at[nx - 1])
        x_in[x, d, j] = joined(x)

    def fold(d, j, parts, decays, size):
        running = None
        for c in members(d, size):
            part = parts[c, d, j]
            running = part if running is None else decays[c, mine + j] * running + part
        return running

    def up_x(n, d, j):
        if n == 0:
            landed(d_x.at[pl.ds(0, nx - 1)], r_d.at[1])
            product = d_x[0]
            for c in range(1, nx):
                product = product * d_x[c]
            d_y[y] = product
            for o in ys:
                go(d_y.at[y], d_y.at[y], s_d, r_d.at[2], y_id(o))
        landed(x_in.at[pl.ds(0, nx - 1), d, j], r_x.at[n])
        row_tot[d, j] = fold(d, j, x_in, d_x, nx)
        for o in ys:
            go(row_tot.at[d, j, rows_of(o, wy), :], y_in.at[y, d, j], s_y, r_y.at[n], y_id(o))
        y_in[y, d, j] = row_tot[d, j, rows_of(y, wy), :]

    def up_y(n, d, j):
        if n == 0:
            if ny > 1:
                landed(d_y.at[pl.ds(0, ny - 1)], r_d.at[2])
            product = d_y[0]
            for c in range(1, ny):
                product = product * d_y[c]
            d_z[z] = product
            if nz > 1:
                hear(1, CORES * (nz - 1))
                learn(1)
            for t in zs:
                go(d_z.at[z], d_z.at[z], s_d, r_d.at[3], z_id(t))
        if ny > 1:
            landed(y_in.at[pl.ds(0, ny - 1), d, j], r_y.at[n])
        plane_tot[d, j] = fold(d, j, y_in, d_y, ny)
        send_z(n, d, j, 0, plane_tot.at[d, j])

    levels = (nz - 1).bit_length()
    shared = max(0, levels - 2)

    def place(d):
        return z if d == 0 else nz - 1 - z

    def z_sends(d, level):
        size, p = 1 << level, place(d)
        last = lax.rem(p, 2 * size) == size - 1
        return [(i + 1, jnp.logical_and(last, p + i + 1 < nz)) for i in range(size)]

    def z_hears(d, level):
        return lax.rem(place(d), 2 << level) >= 1 << level

    def send_z(n, d, j, level, src):
        if level < levels:
            for hop, needed in z_sends(d, level):
                to = lax.rem(z + hop, nz) if d == 0 else lax.rem(z - hop + nz, nz)
                c = copy(src, z_in.at[2 * level + d, j], s_z, r_z.at[min(level, shared), n], z_id(to))
                pl.when(needed)(c.start)

    def z_weight(d, level):
        size = 1 << level
        start = place(d) // size * size
        weight = jnp.ones_like(d_core[...])
        for i in range(size - 1):
            q = lax.rem(start + i, nz)
            passed = d_z[q if d == 0 else nz - 1 - q]
            weight = jnp.where(start + i < place(d), weight * passed, weight)
        return weight

    def spread(d, j, held, parts, decays, size, out):
        last = members(d, size)[-1]
        for c in members(d, size):
            out[c, d, j] = held
            if c != last:
                held = decays[c, mine + j] * held + parts[c, d, j]

    def over_z(level, n, d, j):
        if n == 0 and level == 0:
            landed(d_z.at[pl.ds(0, nz - 1)], r_d.at[3])
            for side in range(2):
                for upper in range(levels):
                    weights[upper, side] = z_weight(side, upper)
        if level == 0:
            z_carry[d, j] = jnp.zeros((wy, DV), F32)

        def hear_z():
            came = z_in[2 * level + d, j]
            if level:
                came = weights[level, d, mine + j] * came + z_carry[d, j]
            z_carry[d, j] = came

        hears = z_hears(d, level)
        if level == levels - 1 and level:
            both = jnp.logical_and(hears, z_hears(d, level - 1))

            @pl.when(both)
            def _():
                landed(z_in.at[pl.ds(0, 2), j], r_z.at[shared, n])
                early = z_in[2 * (level - 1) + d, j]
                if level > 1:
                    early = weights[level - 1, d, mine + j] * early + z_carry[d, j]
                z_carry[d, j] = early
                hear_z()

            @pl.when(jnp.logical_and(hears, jnp.logical_not(both)))
            def _():
                landed(z_in.at[2 * level + d, j], r_z.at[shared, n])
                hear_z()
        else:
            alone = hears
            if level == levels - 2:
                alone = jnp.logical_and(hears, jnp.logical_not(z_hears(d, level + 1)))

            @pl.when(alone)
            def _():
                landed(z_in.at[2 * level + d, j], r_z.at[level, n])
                hear_z()

        if level + 1 < levels:
            @pl.when(z_sends(d, level + 1)[0][1])
            def _():
                z_out[level, d, j] = d_z[z, mine + j] * z_carry[d, j] + plane_tot[d, j]

            send_z(n, d, j, level + 1, z_out.at[level, d, j])

    def down_z(n, d, j):
        if levels:
            over_z(levels - 1, n, d, j)
        else:
            z_carry[d, j] = jnp.zeros((wy, DV), F32)
        spread(d, j, z_carry[d, j], y_in, d_y, ny, y_out)
        send_y(n, d, j)

    def send_y(n, d, j):
        for o in ys:
            go(y_out.at[o, d, j], row_carry.at[d, j, rows_of(y, wy), :], s_yout, r_yout.at[n], y_id(o))
        row_carry[d, j, rows_of(y, wy), :] = y_out[y, d, j]

    def starts(d, at):
        row = jnp.logical_and(z == (0 if d == 0 else nz - 1), y == (0 if d == 0 else ny - 1))
        return jnp.logical_and(row, at == (0 if d == 0 else nx - 1))

    final = len(chunks) - 1

    def send_x(n, d, j, part=None, ready=True):
        size = wx if part is None else wx // 2
        start = 0 if part is None else part * size
        sem = r_tail if part == 1 else r_xout.at[n]
        for o in xs:
            c = copy(
                x_out.at[o, d, j, pl.ds(start, size), :],
                carry.at[d, j, pl.ds(pl.multiple_of(x * wx + start, size), size), :],
                s_xout.at[d], sem, x_id(o),
            )
            pl.when(jnp.logical_and(jnp.logical_not(starts(d, o)), ready))(c.start)

    def down_y(n, d, j):
        if ny > 1:
            landed(row_carry.at[d, j, pl.ds(0, (ny - 1) * wy), :], r_yout.at[n])
        spread(d, j, row_carry[d, j], x_in, d_x, nx, x_out)
        if n == final:
            for part in range(2):
                send_x(n, d, j, part, core == 0)
        else:
            send_x(n, d, j)
        carry[d, j, rows_of(x, wx), :] = x_out[x, d, j]
        if n == final:
            send_back(n, d, j, rows_of(x, wx))

    def down_x(n, d, j):
        starting = starts(d, x)

        def come(ref, sem):
            @pl.when(starting)
            def _():
                for o in xs:
                    carry[d, j, rows_of(o, wx), :] = jnp.zeros((wx, DV), F32)

            pl.when(jnp.logical_not(starting))(lambda: landed(ref, sem))

        if n == final:
            size = wx // 2
            for part in range(2):
                come(carry.at[d, j, pl.ds(0, (nx - 1) * size), :], r_tail if part else r_xout.at[n])
                for o in xs:
                    start = pl.multiple_of(o * wx + part * size, size)
                    send_back(n, d, j, pl.ds(start, size))
        else:
            come(carry.at[d, j, pl.ds(0, (nx - 1) * wx), :], r_xout.at[n])
            if n == final - 1:
                send_x(final, *chunks[final], 0, core != 0)
            send_back(n, d, j, pl.ds(0, DK))
        outer(d, mine + j)

    def send_back(n, d, j, part):
        near = first if d == 0 else jnp.logical_not(first)

        @pl.when(near)
        def _():
            got = carry[d, j, part, :]
            back_buf[d, j, part, :] = d_core[mine + j] * got + total_buf[d, mine + j, part, :]
            from_buf[d, mine + j, part, :] = got

        @pl.when(jnp.logical_not(near))
        def _():
            got = carry[d, j, part, :]
            back_buf[d, j, part, :] = got
            from_buf[d, mine + j, part, :] = d_mate[mine + j] * got + peer_buf[d, j, part, :]

        go(back_buf.at[d, j, part, :], from_buf.at[d, mine + j, part, :], s_back, r_back.at[n], mate)

    def finish(n, d, j):
        landed(from_buf.at[d, theirs + j], r_back.at[n])
        outer(d, theirs + j)

    def load_more(k):
        for head in (theirs + k, mine + k):
            load(head, 0, k + 2)
            load(head, 1, k + 2)

    def greet_mate():
        go(d_core, d_mate, s_d, r_d.at[0], mate)
        send_core(0, *chunks[0])

    totals = (forward_total, reverse_total)
    ready(0, 2, 1)
    forward_total(theirs)
    hear(0, 1 + CORES * (nx + ny - 2))
    pl.when(core == 0)(greet_mate)
    ready(2, 2, 1)
    forward_total(mine)
    learn(0)
    pl.when(core != 0)(greet_mate)
    load_more(1)
    ready(1, 4, 1)
    reverse_total(theirs)
    send_core(1, *chunks[1])
    landed(d_mate, r_d.at[0])
    d_x[x] = d_core[...] * d_mate[...]
    for o in xs:
        go(d_x.at[x], d_x.at[x], s_d, r_d.at[1], x_id(o))
    join_cores(0, *chunks[0])
    for k in range(2, half):
        load_more(k)
    reverse_total(mine)
    join_cores(1, *chunks[1])
    late, held = [], {0}
    for turn in (range(n, n + 2) for n in range(2, len(chunks), 2)):
        for n in turn:
            d, k = chunks[n]
            if k not in held:
                ready(k + 2, 4, CORES)
                held.add(k)
            totals[d](theirs + k)
            send_core(n, d, k)
            for m in late:
                join_cores(m, *chunks[m])
            late = []
        for n in turn:
            totals[chunks[n][0]](mine + chunks[n][1])
        join_cores(turn[0], *chunks[turn[0]])
        late = turn[1:]
    for m in late:
        join_cores(m, *chunks[m])

    def inside(n, d, j):
        for h in range(n, HEAD_COUNT, len(chunks)):
            intra(h)

    climb = [(2 + level, functools.partial(over_z, level)) for level in range(levels - 1)]
    top = 2 + len(climb)
    back = len(chunks)
    stages = [(0, up_x), (0, inside), (top + 3, down_y), (back + 2, finish), (back, down_x)]
    stages += [(1, up_y)] + climb + [(top + 1, down_z)]
    for slot in range(2 * len(chunks) + 1):
        for lag, stage in stages:
            n = slot - lag
            if stage is finish and n >= final - 1:
                n = final
            if 0 <= n < len(chunks):
                stage(n, *chunks[n])
            if stage is finish and n == final - 2:
                send_x(final, *chunks[final], 1, core != 0)
                finish(final - 1, *chunks[final - 1])

    left(peer_buf, s_core)
    left(x_in.at[pl.ds(0, nx - 1)], s_x)
    withheld = [
        sum(jnp.where(starts(d, o), 1, 0) for o in xs) for d in range(2)
    ]
    for d in range(2):
        for amount in (nx - 2, nx - 1):
            if amount:
                pl.when(withheld[d] == nx - 1 - amount)(
                    functools.partial(left, x_out.at[pl.ds(0, amount), d], s_xout.at[d])
                )
    left(back_buf, s_back)
    left(decay_rows.at[pl.ds(0, nx + ny + nz - 2)], s_d)
    if ny > 1:
        left(y_in.at[pl.ds(0, ny - 1)], s_y)
        left(y_out.at[pl.ds(0, ny - 1)], s_yout)
    if nz > 1:
        sends = sum(
            jnp.where(needed, 1, 0)
            for level in range(levels) for d in range(2) for _, needed in z_sends(d, level)
        )
        for amount in range(1, nz):
            pl.when(sends == amount)(functools.partial(left, z_in.at[pl.ds(0, amount)], s_z))


def write_kernel(gq_ref, gk_ref, gv_ref, gq_hbm, gk_hbm, gv_hbm, sems):
    copies = [
        pltpu.make_async_copy(near, far, sems.at[i])
        for i, (near, far) in enumerate(((gq_ref, gq_hbm), (gk_ref, gk_hbm), (gv_ref, gv_hbm)))
    ]
    for c in copies:
        c.start()
    for c in copies:
        c.wait()


def body(nx, ny, nz, queries, keys, values, grad_out, log_decay):
    tokens = queries.shape[0]
    count = tokens // BLOCK
    half = HEAD_COUNT // CORES
    wx = DK // nx
    wy = wx // ny
    levels = (nz - 1).bit_length()
    n = 2 * half
    vm = pl.BlockSpec(memory_space=pltpu.VMEM)
    hbm = pl.BlockSpec(memory_space=pltpu.HBM)
    dma = pltpu.SemaphoreType.DMA

    def states(*lead):
        return pltpu.VMEM(lead + (DV,), F32)

    def decays(*lead):
        return pltpu.VMEM(lead + (HEAD_COUNT, 1, DV), F32)

    out = jax.ShapeDtypeStruct((tokens, HEAD_COUNT * DK), BF16)
    near = pltpu.VMEM(out.shape, out.dtype)
    grads = pl.pallas_call(
        functools.partial(retention_kernel, nx, ny, nz),
        out_shape=(near, near, near),
        in_specs=[hbm] * 5,
        out_specs=(vm, vm, vm),
        scratch_shapes=[
            pltpu.VMEM((HEAD_COUNT, tokens), F32),
            pltpu.VMEM((4, tokens, HEAD_COUNT * DK), BF16),
            pltpu.VMEM((count, HEAD_COUNT, 1, BLOCK), F32),
            states(2, max(1, count - 1), HEAD_COUNT, DK),
            states(3, HEAD_COUNT, tokens),
            states(2, HEAD_COUNT, DK), states(2, HEAD_COUNT, DK),
            states(2, half, DK), states(2, half, DK),
            states(2, half, DK), states(nx, 2, half, wx), states(2, half, wx),
            states(ny, 2, half, wy), states(2, half, wy),
            states(max(2 * levels, nz), half, wy), states(max(1, levels - 1), 2, half, wy), states(2, half, wy),
            states(ny, 2, half, wy), states(2, half, wx),
            states(nx, 2, half, wx), states(2, half, DK),
            decays(2 + nx + ny + nz), decays(max(1, levels), 2), pltpu.SemaphoreType.REGULAR, dma, dma((half + 2,)),
            dma, dma((half,)), dma((nx,)), dma, dma((n,)), dma, dma((n,)), dma, dma((max(1, levels - 1), n)),
            dma, dma((n,)), dma((2,)), dma((n,)), dma, dma, dma((n,)), dma, dma((4,)),
        ],
        compiler_params=pltpu.CompilerParams(collective_id=0, has_side_effects=True, vmem_limit_bytes=52 << 20),
        name="retention",
    )(pltpu.with_memory_space_constraint(log_decay, pltpu.HBM), queries, keys, values, grad_out)
    return pl.pallas_call(
        write_kernel,
        out_shape=(out, out, out),
        in_specs=[vm] * 3,
        out_specs=(hbm, hbm, hbm),
        scratch_shapes=[dma((3,))],
        name="write",
    )(*(pltpu.with_memory_space_constraint(g, pltpu.VMEM) for g in grads))


def solution(mesh):
    nx = mesh.shape["mem"] // CORES
    ny = nx if mesh.shape["grp"] % nx == 0 else 1
    nz = mesh.shape["grp"] // ny
    tokens = P(("grp", "mem"), None)
    return jax.shard_map(
        functools.partial(body, nx, ny, nz),
        mesh=mesh,
        in_specs=(tokens, tokens, tokens, tokens, P(None, ("grp", "mem"))),
        out_specs=(tokens, tokens, tokens),
        check_vma=False,
    )
```

```python
import functools

import jax
import jax.numpy as jnp
from jax import lax
from jax.experimental import pallas as pl
from jax.experimental.pallas import tpu as pltpu
from jax.sharding import PartitionSpec as P

HEAD_COUNT = 8
DK = 256
DV = 256
BLOCK = 128
CORES = 2
KEYS, VALUES, QUERIES, GRADS = range(4)
MESH = pl.DeviceIdType.MESH
F32 = jnp.float32
BF16 = jnp.bfloat16


def dot(a, b, ca, cb):
    return lax.dot_general(a, b, (((ca,), (cb,)), ((), ())), preferred_element_type=F32)


def spread_rows(row):
    flat = jnp.broadcast_to(row, (BLOCK, BLOCK))
    return flat, flat.T


def wide(mat, width):
    return jnp.concatenate([mat] * (width // BLOCK), axis=1)


def retention_kernel(
    nx, ny, nz, logs_hbm, q_hbm, k_hbm, v_hbm, g_hbm, gq_ref, gk_ref, gv_ref,
    logs_ref, toks, cum, local, inner, total_buf, from_buf, peer_buf, back_buf,
    chip_buf, x_in, row_tot, y_in, plane_tot, z_in, z_out, z_carry, y_out, row_carry, x_out, carry,
    decay_rows, weights, s_meet, s_logs, s_in, s_core, r_core, r_first, s_x, r_x, s_y, r_y, s_z, r_z,
    s_yout, r_yout, s_xout, r_xout, r_tail, s_back, r_back, s_d, r_d,
):
    count = logs_ref.shape[1] // BLOCK
    scale = DK ** (-0.5)
    half = HEAD_COUNT // CORES
    wx = DK // nx
    wy = wx // ny
    d_core, d_mate = decay_rows.at[0], decay_rows.at[1]
    d_x, d_y = decay_rows.at[pl.ds(2, nx)], decay_rows.at[pl.ds(2 + nx, ny)]
    d_z = decay_rows.at[pl.ds(2 + nx + ny, nz)]
    early = max(1, half - 2)
    chunks = [(d, k) for k in range(early) for d in range(2)]
    chunks += [(d, k) for d in (1, 0) for k in range(early, half)]
    grp, mem = lax.axis_index("grp"), lax.axis_index("mem")
    z, y = grp // ny, lax.rem(grp, ny)
    x, core = mem // CORES, lax.rem(mem, CORES)
    mate = (grp, x * CORES + 1 - core)

    def x_id(to):
        return (grp, to * CORES + core)

    def y_id(to):
        return (z * ny + to, mem)

    def z_id(to):
        return (to * ny + y, mem)

    xs = [lax.rem(x + off, nx) for off in range(1, nx)]
    ys = [lax.rem(y + off, ny) for off in range(1, ny)]
    zs = [lax.rem(z + off, nz) for off in range(1, nz)]
    barrier = pltpu.get_barrier_semaphore()

    def tell(sem, device):
        pl.semaphore_signal(sem, inc=1, device_id=device, device_id_type=MESH)

    for device in [(grp, o * CORES) for o in xs] + [(z * ny + o, x * CORES) for o in ys]:
        tell(barrier, device)
    pl.when(core == 1)(lambda: tell(barrier, mate))
    for o in zs:
        tell(barrier, (o * ny + y, x * CORES + 1))

    def hear(hearer, signals):
        @pl.when(core == hearer)
        def _():
            pl.semaphore_wait(barrier, signals)
            tell(s_meet, mate)

    def learn(hearer):
        @pl.when(core != hearer)
        def _():
            pl.semaphore_wait(s_meet, 1)

    def copy(src, dst, send, recv, device):
        return pltpu.make_async_remote_copy(
            src_ref=src, dst_ref=dst, send_sem=send, recv_sem=recv,
            device_id=device, device_id_type=MESH,
        )

    def go(*args):
        copy(*args).start()

    def landed(ref, sem):
        copy(ref, ref, s_back, sem, mate).wait_recv()

    def left(ref, sem):
        copy(ref, ref, sem, r_back.at[0], mate).wait_send()

    def members(d, size):
        return range(size) if d == 0 else range(size - 1, -1, -1)

    mine, theirs = core * half, (1 - core) * half

    def rows_of(c, size):
        return pl.ds(pl.multiple_of(c * size, size), size)

    def cols_of(head, size):
        return pl.ds(pl.multiple_of(head * size, size), size)

    def tokens_of(b):
        return pl.ds(b * BLOCK, BLOCK)

    load_logs = pltpu.make_async_copy(logs_hbm, logs_ref, s_logs)
    load_logs.start()

    def load(head, pair, slot):
        part = cols_of(head, DK)
        for i in (2 * pair, 2 * pair + 1):
            far = (k_hbm, v_hbm, q_hbm, g_hbm)[i]
            pltpu.make_async_copy(far.at[:, part], toks.at[i, :, part], s_in.at[slot]).start()

    load(theirs, 0, 0)

    def ready(slot, parts, heads):
        held = toks.at[pl.ds(0, parts), :, pl.ds(0, heads * DK)]
        pltpu.make_async_copy(held, held, s_in.at[slot]).wait()

    def tok(i, head, b):
        return toks[i, tokens_of(b), cols_of(head, DK)]

    square = (BLOCK, BLOCK)
    lower = lax.broadcasted_iota(jnp.int32, square, 0) >= lax.broadcasted_iota(jnp.int32, square, 1)
    ones = jnp.where(lower, 1.0, 0.0)
    load_logs.wait()
    load(mine, 0, 2)
    load(theirs, 1, 1)
    load(mine, 1, 1)
    carried = None
    for b in range(count):
        row = lax.dot_general(
            logs_ref[:, b * BLOCK:(b + 1) * BLOCK], ones, (((1,), (1,)), ((), ())),
            precision=lax.Precision.HIGHEST, preferred_element_type=F32,
        )
        for h in range(HEAD_COUNT):
            cum[b, h] = row[h:h + 1, :]
        whole = jnp.exp(row[:, BLOCK - 1:BLOCK])
        carried = whole if carried is None else carried * whole
    carried = jnp.broadcast_to(carried, (HEAD_COUNT, DV))
    for h in range(HEAD_COUNT):
        d_core[h] = carried[h:h + 1, :]
    def factors(head, b):
        row = cum[b, head]
        flat, cols = spread_rows(row)
        end = row[:, BLOCK - 1:BLOCK]
        return flat, cols, end

    def forward_total(head):
        forward = None
        for b in range(count):
            _, cols, end = factors(head, b)
            kd = tok(KEYS, head, b).astype(F32) * wide(jnp.exp(end - cols), DK)
            whole = jnp.broadcast_to(jnp.exp(end), (1, DV))
            part = dot(kd.astype(BF16), tok(VALUES, head, b), 0, 0)
            if b > 0:
                local[0, b - 1, head] = forward
            forward = part if forward is None else whole * forward + part
        total_buf[0, head] = forward

    def reverse_total(head):
        back = None
        for b in reversed(range(count)):
            _, cols, end = factors(head, b)
            qd = tok(QUERIES, head, b).astype(F32) * wide(jnp.exp(cols), DK)
            whole = jnp.broadcast_to(jnp.exp(end), (1, DV))
            part = dot(qd.astype(BF16), tok(GRADS, head, b), 0, 0)
            if b < count - 1:
                local[1, b, head] = back
            back = part if back is None else whole * back + part
        total_buf[1, head] = back

    def intra(head):
        for b in range(count):
            flat, cols, _ = factors(head, b)
            decay = jnp.where(lower, jnp.exp(jnp.where(lower, cols - flat, 0.0)), 0.0)
            q, k = tok(QUERIES, head, b), tok(KEYS, head, b)
            v, g = tok(VALUES, head, b), tok(GRADS, head, b)
            wg = (dot(g, v, 1, 1) * decay).astype(BF16)
            wv = (dot(q, k, 1, 1) * decay).astype(BF16)
            inner[0, head, tokens_of(b), :] = dot(wg, k, 1, 0)
            inner[1, head, tokens_of(b), :] = dot(wg, q, 0, 0)
            inner[2, head, tokens_of(b), :] = dot(wv, g, 0, 0)

    def outer(d, head):
        coming = from_buf[d, head]
        weight = None
        for step, b in enumerate(members(d, count)):
            _, cols, end = factors(head, b)
            if step == 0:
                low = coming.astype(BF16)
            else:
                low = (local[d, b - 1 if d == 0 else b, head] + weight * coming).astype(BF16)
            whole = jnp.broadcast_to(jnp.exp(end), (1, DV))
            weight = whole if weight is None else weight * whole
            if d == 0:
                far = wide(jnp.exp(cols), DK) * dot(tok(GRADS, head, b), low, 1, 1)
                near = inner[0, head, tokens_of(b), :]
                gq_ref[tokens_of(b), cols_of(head, DK)] = (scale * (near + far)).astype(BF16)
            else:
                tail = wide(jnp.exp(end - cols), DK)
                near = inner[1, head, tokens_of(b), :]
                far = tail * dot(tok(VALUES, head, b), low, 1, 1)
                gk_ref[tokens_of(b), cols_of(head, DK)] = (scale * (near + far)).astype(BF16)
                near = inner[2, head, tokens_of(b), :]
                far = tail * dot(tok(KEYS, head, b), low, 1, 0)
                gv_ref[tokens_of(b), cols_of(head, DV)] = (scale * (near + far)).astype(BF16)

    first = core == 0

    def send_core(n, d, j):
        if n:
            go(total_buf.at[d, theirs + j], peer_buf.at[d, j], s_core, r_core.at[n // 2], mate)
        else:
            for i, o in enumerate(xs + [x]):
                part = rows_of(o, wx)
                go(total_buf.at[d, theirs + j, part, :], peer_buf.at[d, j, part, :],
                   s_core, r_first.at[i], mate)

    def join_cores(n, d, j):
        if n == 1:
            landed(peer_buf.at[d, j], r_core.at[0])
        elif n and n % 2 == 0:
            landed(peer_buf.at[0, pl.ds(0, 2)], r_core.at[n // 2])
        own_d, peer_d = d_core[mine + j], d_mate[mine + j]
        one = jnp.ones_like(own_d)
        if d == 0:
            w_own, w_peer = jnp.where(first, peer_d, one), jnp.where(first, one, own_d)
        else:
            w_own, w_peer = jnp.where(first, one, peer_d), jnp.where(first, own_d, one)

        def joined(o):
            part = rows_of(o, wx)
            return w_own * total_buf[d, mine + j, part, :] + w_peer * peer_buf[d, j, part, :]

        for i, o in enumerate(xs):
            if n == 0:
                landed(peer_buf.at[d, j, rows_of(o, wx), :], r_first.at[i])
            chip_buf[d, j, rows_of(o, wx), :] = joined(o)
            go(chip_buf.at[d, j, rows_of(o, wx), :], x_in.at[x, d, j], s_x, r_x.at[n], x_id(o))
        if n == 0:
            landed(peer_buf.at[d, j, rows_of(x, wx), :], r_first.at[nx - 1])
        x_in[x, d, j] = joined(x)

    def fold(d, j, parts, decays, size):
        running = None
        for c in members(d, size):
            part = parts[c, d, j]
            running = part if running is None else decays[c, mine + j] * running + part
        return running

    def up_x(n, d, j):
        if n == 0:
            landed(d_x.at[pl.ds(0, nx - 1)], r_d.at[1])
            product = d_x[0]
            for c in range(1, nx):
                product = product * d_x[c]
            d_y[y] = product
            for o in ys:
                go(d_y.at[y], d_y.at[y], s_d, r_d.at[2], y_id(o))
        landed(x_in.at[pl.ds(0, nx - 1), d, j], r_x.at[n])
        row_tot[d, j] = fold(d, j, x_in, d_x, nx)
        for o in ys:
            go(row_tot.at[d, j, rows_of(o, wy), :], y_in.at[y, d, j], s_y, r_y.at[n], y_id(o))
        y_in[y, d, j] = row_tot[d, j, rows_of(y, wy), :]

    def up_y(n, d, j):
        if n == 0:
            if ny > 1:
                landed(d_y.at[pl.ds(0, ny - 1)], r_d.at[2])
            product = d_y[0]
            for c in range(1, ny):
                product = product * d_y[c]
            d_z[z] = product
            if nz > 1:
                hear(1, CORES * (nz - 1))
                learn(1)
            for t in zs:
                go(d_z.at[z], d_z.at[z], s_d, r_d.at[3], z_id(t))
        if ny > 1:
            landed(y_in.at[pl.ds(0, ny - 1), d, j], r_y.at[n])
        plane_tot[d, j] = fold(d, j, y_in, d_y, ny)
        send_z(n, d, j, 0, plane_tot.at[d, j])

    levels = (nz - 1).bit_length()
    shared = max(0, levels - 2)

    def place(d):
        return z if d == 0 else nz - 1 - z

    def z_sends(d, level):
        size, p = 1 << level, place(d)
        last = lax.rem(p, 2 * size) == size - 1
        return [(i + 1, jnp.logical_and(last, p + i + 1 < nz)) for i in range(size)]

    def z_hears(d, level):
        return lax.rem(place(d), 2 << level) >= 1 << level

    def send_z(n, d, j, level, src):
        if level < levels:
            for hop, needed in z_sends(d, level):
                to = lax.rem(z + hop, nz) if d == 0 else lax.rem(z - hop + nz, nz)
                c = copy(src, z_in.at[2 * level + d, j], s_z, r_z.at[min(level, shared), n], z_id(to))
                pl.when(needed)(c.start)

    def z_weight(d, level):
        size = 1 << level
        start = place(d) // size * size
        weight = jnp.ones_like(d_core[...])
        for i in range(size - 1):
            q = lax.rem(start + i, nz)
            passed = d_z[q if d == 0 else nz - 1 - q]
            weight = jnp.where(start + i < place(d), weight * passed, weight)
        return weight

    def spread(d, j, held, parts, decays, size, out):
        last = members(d, size)[-1]
        for c in members(d, size):
            out[c, d, j] = held
            if c != last:
                held = decays[c, mine + j] * held + parts[c, d, j]

    def over_z(level, n, d, j):
        if n == 0 and level == 0:
            landed(d_z.at[pl.ds(0, nz - 1)], r_d.at[3])
            for side in range(2):
                for upper in range(levels):
                    weights[upper, side] = z_weight(side, upper)
        if level == 0:
            z_carry[d, j] = jnp.zeros((wy, DV), F32)

        def hear_z():
            came = z_in[2 * level + d, j]
            if level:
                came = weights[level, d, mine + j] * came + z_carry[d, j]
            z_carry[d, j] = came

        hears = z_hears(d, level)
        if level == levels - 1 and level:
            both = jnp.logical_and(hears, z_hears(d, level - 1))

            @pl.when(both)
            def _():
                landed(z_in.at[pl.ds(0, 2), j], r_z.at[shared, n])
                early = z_in[2 * (level - 1) + d, j]
                if level > 1:
                    early = weights[level - 1, d, mine + j] * early + z_carry[d, j]
                z_carry[d, j] = early
                hear_z()

            @pl.when(jnp.logical_and(hears, jnp.logical_not(both)))
            def _():
                landed(z_in.at[2 * level + d, j], r_z.at[shared, n])
                hear_z()
        else:
            alone = hears
            if level == levels - 2:
                alone = jnp.logical_and(hears, jnp.logical_not(z_hears(d, level + 1)))

            @pl.when(alone)
            def _():
                landed(z_in.at[2 * level + d, j], r_z.at[level, n])
                hear_z()

        if level + 1 < levels:
            @pl.when(z_sends(d, level + 1)[0][1])
            def _():
                z_out[level, d, j] = d_z[z, mine + j] * z_carry[d, j] + plane_tot[d, j]

            send_z(n, d, j, level + 1, z_out.at[level, d, j])

    def down_z(n, d, j):
        if levels:
            over_z(levels - 1, n, d, j)
        else:
            z_carry[d, j] = jnp.zeros((wy, DV), F32)
        spread(d, j, z_carry[d, j], y_in, d_y, ny, y_out)
        send_y(n, d, j)

    def send_y(n, d, j):
        for o in ys:
            go(y_out.at[o, d, j], row_carry.at[d, j, rows_of(y, wy), :], s_yout, r_yout.at[n], y_id(o))
        row_carry[d, j, rows_of(y, wy), :] = y_out[y, d, j]

    def starts(d, at):
        row = jnp.logical_and(z == (0 if d == 0 else nz - 1), y == (0 if d == 0 else ny - 1))
        return jnp.logical_and(row, at == (0 if d == 0 else nx - 1))

    final = len(chunks) - 1

    def send_x(n, d, j, part=None, ready=True):
        size = wx if part is None else wx // 2
        start = 0 if part is None else part * size
        sem = r_tail if part == 1 else r_xout.at[n]
        for o in xs:
            c = copy(
                x_out.at[o, d, j, pl.ds(start, size), :],
                carry.at[d, j, pl.ds(pl.multiple_of(x * wx + start, size), size), :],
                s_xout.at[d], sem, x_id(o),
            )
            pl.when(jnp.logical_and(jnp.logical_not(starts(d, o)), ready))(c.start)

    held_late = jnp.logical_and(core != 0, starts(1, x))
    held_soon = jnp.logical_and(core != 0, jnp.logical_not(starts(1, x)))

    def down_y(n, d, j):
        if ny > 1:
            landed(row_carry.at[d, j, pl.ds(0, (ny - 1) * wy), :], r_yout.at[n])
        spread(d, j, row_carry[d, j], x_in, d_x, nx, x_out)
        if n == final:
            for part in range(2):
                send_x(n, d, j, part, core == 0)
        else:
            send_x(n, d, j)
        carry[d, j, rows_of(x, wx), :] = x_out[x, d, j]
        if n == final:
            send_back(n, d, j, rows_of(x, wx))

    def down_x(n, d, j):
        starting = starts(d, x)

        def come(ref, sem):
            @pl.when(starting)
            def _():
                for o in xs:
                    carry[d, j, rows_of(o, wx), :] = jnp.zeros((wx, DV), F32)

            pl.when(jnp.logical_not(starting))(lambda: landed(ref, sem))

        if n == final:
            size = wx // 2
            for part in range(2):
                come(carry.at[d, j, pl.ds(0, (nx - 1) * size), :], r_tail if part else r_xout.at[n])
                for o in xs:
                    start = pl.multiple_of(o * wx + part * size, size)
                    send_back(n, d, j, pl.ds(start, size))
        else:
            come(carry.at[d, j, pl.ds(0, (nx - 1) * wx), :], r_xout.at[n])
            if n == final - 1:
                send_x(final, *chunks[final], 0, held_soon)
            send_back(n, d, j, pl.ds(0, DK))
        outer(d, mine + j)

    def send_back(n, d, j, part):
        near = first if d == 0 else jnp.logical_not(first)

        @pl.when(near)
        def _():
            got = carry[d, j, part, :]
            back_buf[d, j, part, :] = d_core[mine + j] * got + total_buf[d, mine + j, part, :]
            from_buf[d, mine + j, part, :] = got

        @pl.when(jnp.logical_not(near))
        def _():
            got = carry[d, j, part, :]
            back_buf[d, j, part, :] = got
            from_buf[d, mine + j, part, :] = d_mate[mine + j] * got + peer_buf[d, j, part, :]

        go(back_buf.at[d, j, part, :], from_buf.at[d, mine + j, part, :], s_back, r_back.at[n], mate)

    def finish(n, d, j):
        landed(from_buf.at[d, theirs + j], r_back.at[n])
        outer(d, theirs + j)

    def load_more(k):
        for head in (theirs + k, mine + k):
            load(head, 0, k + 2)
            load(head, 1, k + 2)

    def greet_mate():
        go(d_core, d_mate, s_d, r_d.at[0], mate)
        send_core(0, *chunks[0])

    totals = (forward_total, reverse_total)
    ready(0, 2, 1)
    forward_total(theirs)
    hear(0, 1 + CORES * (nx + ny - 2))
    pl.when(core == 0)(greet_mate)
    ready(2, 2, 1)
    forward_total(mine)
    learn(0)
    pl.when(core != 0)(greet_mate)
    load_more(1)
    ready(1, 4, 1)
    reverse_total(theirs)
    send_core(1, *chunks[1])
    landed(d_mate, r_d.at[0])
    d_x[x] = d_core[...] * d_mate[...]
    for o in xs:
        go(d_x.at[x], d_x.at[x], s_d, r_d.at[1], x_id(o))
    join_cores(0, *chunks[0])
    for k in range(2, half):
        load_more(k)
    reverse_total(mine)
    join_cores(1, *chunks[1])
    late, held = [], {0}
    for turn in (range(n, n + 2) for n in range(2, len(chunks), 2)):
        for n in turn:
            d, k = chunks[n]
            if k not in held:
                ready(k + 2, 4, CORES)
                held.add(k)
            totals[d](theirs + k)
            send_core(n, d, k)
            for m in late:
                join_cores(m, *chunks[m])
            late = []
        for n in turn:
            totals[chunks[n][0]](mine + chunks[n][1])
        join_cores(turn[0], *chunks[turn[0]])
        late = turn[1:]
    for m in late:
        join_cores(m, *chunks[m])

    def inside(n, d, j):
        for h in range(n, HEAD_COUNT, len(chunks)):
            intra(h)

    climb = [(2 + level, functools.partial(over_z, level)) for level in range(levels - 1)]
    top = 2 + len(climb)
    back = len(chunks)
    stages = [(0, up_x), (0, inside), (top + 3, down_y), (back + 2, finish), (back, down_x)]
    stages += [(1, up_y)] + climb + [(top + 1, down_z)]
    for slot in range(2 * len(chunks) + 1):
        for lag, stage in stages:
            n = slot - lag
            if stage is finish and n >= final - 1:
                n = final
            if 0 <= n < len(chunks):
                stage(n, *chunks[n])
            if stage is finish and n == final - 2:
                send_x(final, *chunks[final], 0, held_late)
                send_x(final, *chunks[final], 1, held_soon)
                finish(final - 1, *chunks[final - 1])
                send_x(final, *chunks[final], 1, held_late)

    left(peer_buf, s_core)
    left(x_in.at[pl.ds(0, nx - 1)], s_x)
    withheld = [
        sum(jnp.where(starts(d, o), 1, 0) for o in xs) for d in range(2)
    ]
    for d in range(2):
        for amount in (nx - 2, nx - 1):
            if amount:
                pl.when(withheld[d] == nx - 1 - amount)(
                    functools.partial(left, x_out.at[pl.ds(0, amount), d], s_xout.at[d])
                )
    left(back_buf, s_back)
    left(decay_rows.at[pl.ds(0, nx + ny + nz - 2)], s_d)
    if ny > 1:
        left(y_in.at[pl.ds(0, ny - 1)], s_y)
        left(y_out.at[pl.ds(0, ny - 1)], s_yout)
    if nz > 1:
        sends = sum(
            jnp.where(needed, 1, 0)
            for level in range(levels) for d in range(2) for _, needed in z_sends(d, level)
        )
        for amount in range(1, nz):
            pl.when(sends == amount)(functools.partial(left, z_in.at[pl.ds(0, amount)], s_z))


def write_kernel(gq_ref, gk_ref, gv_ref, gq_hbm, gk_hbm, gv_hbm, sems):
    copies = [
        pltpu.make_async_copy(near, far, sems.at[i])
        for i, (near, far) in enumerate(((gq_ref, gq_hbm), (gk_ref, gk_hbm), (gv_ref, gv_hbm)))
    ]
    for c in copies:
        c.start()
    for c in copies:
        c.wait()


def body(nx, ny, nz, queries, keys, values, grad_out, log_decay):
    tokens = queries.shape[0]
    count = tokens // BLOCK
    half = HEAD_COUNT // CORES
    wx = DK // nx
    wy = wx // ny
    levels = (nz - 1).bit_length()
    n = 2 * half
    vm = pl.BlockSpec(memory_space=pltpu.VMEM)
    hbm = pl.BlockSpec(memory_space=pltpu.HBM)
    dma = pltpu.SemaphoreType.DMA

    def states(*lead):
        return pltpu.VMEM(lead + (DV,), F32)

    def decays(*lead):
        return pltpu.VMEM(lead + (HEAD_COUNT, 1, DV), F32)

    out = jax.ShapeDtypeStruct((tokens, HEAD_COUNT * DK), BF16)
    near = pltpu.VMEM(out.shape, out.dtype)
    grads = pl.pallas_call(
        functools.partial(retention_kernel, nx, ny, nz),
        out_shape=(near, near, near),
        in_specs=[hbm] * 5,
        out_specs=(vm, vm, vm),
        scratch_shapes=[
            pltpu.VMEM((HEAD_COUNT, tokens), F32),
            pltpu.VMEM((4, tokens, HEAD_COUNT * DK), BF16),
            pltpu.VMEM((count, HEAD_COUNT, 1, BLOCK), F32),
            states(2, max(1, count - 1), HEAD_COUNT, DK),
            states(3, HEAD_COUNT, tokens),
            states(2, HEAD_COUNT, DK), states(2, HEAD_COUNT, DK),
            states(2, half, DK), states(2, half, DK),
            states(2, half, DK), states(nx, 2, half, wx), states(2, half, wx),
            states(ny, 2, half, wy), states(2, half, wy),
            states(max(2 * levels, nz), half, wy), states(max(1, levels - 1), 2, half, wy), states(2, half, wy),
            states(ny, 2, half, wy), states(2, half, wx),
            states(nx, 2, half, wx), states(2, half, DK),
            decays(2 + nx + ny + nz), decays(max(1, levels), 2), pltpu.SemaphoreType.REGULAR, dma, dma((half + 2,)),
            dma, dma((half,)), dma((nx,)), dma, dma((n,)), dma, dma((n,)), dma, dma((max(1, levels - 1), n)),
            dma, dma((n,)), dma((2,)), dma((n,)), dma, dma, dma((n,)), dma, dma((4,)),
        ],
        compiler_params=pltpu.CompilerParams(collective_id=0, has_side_effects=True, vmem_limit_bytes=52 << 20),
        name="retention",
    )(pltpu.with_memory_space_constraint(log_decay, pltpu.HBM), queries, keys, values, grad_out)
    return pl.pallas_call(
        write_kernel,
        out_shape=(out, out, out),
        in_specs=[vm] * 3,
        out_specs=(hbm, hbm, hbm),
        scratch_shapes=[dma((3,))],
        name="write",
    )(*(pltpu.with_memory_space_constraint(g, pltpu.VMEM) for g in grads))


def solution(mesh):
    nx = mesh.shape["mem"] // CORES
    ny = nx if mesh.shape["grp"] % nx == 0 else 1
    nz = mesh.shape["grp"] // ny
    tokens = P(("grp", "mem"), None)
    return jax.shard_map(
        functools.partial(body, nx, ny, nz),
        mesh=mesh,
        in_specs=(tokens, tokens, tokens, tokens, P(None, ("grp", "mem"))),
        out_specs=(tokens, tokens, tokens),
        check_vma=False,
    )
```

```python
import functools

import jax
import jax.numpy as jnp
from jax import lax
from jax.experimental import pallas as pl
from jax.experimental.pallas import tpu as pltpu
from jax.sharding import PartitionSpec as P

HEAD_COUNT = 8
DK = 256
DV = 256
BLOCK = 128
CORES = 2
KEYS, VALUES, QUERIES, GRADS = range(4)
MESH = pl.DeviceIdType.MESH
F32 = jnp.float32
BF16 = jnp.bfloat16


def dot(a, b, ca, cb):
    return lax.dot_general(a, b, (((ca,), (cb,)), ((), ())), preferred_element_type=F32)


def spread_rows(row):
    flat = jnp.broadcast_to(row, (BLOCK, BLOCK))
    return flat, flat.T


def wide(mat, width):
    return jnp.concatenate([mat] * (width // BLOCK), axis=1)


def retention_kernel(
    nx, ny, nz, logs_hbm, q_hbm, k_hbm, v_hbm, g_hbm, gq_ref, gk_ref, gv_ref,
    logs_ref, toks, cum, local, inner, total_buf, from_buf, peer_buf, back_buf,
    chip_buf, x_in, row_tot, y_in, plane_tot, z_in, z_out, z_carry, y_out, row_carry, x_out, carry,
    decay_rows, weights, s_meet, s_logs, s_in, s_core, r_core, r_first, s_x, r_x, s_y, r_y, s_z, r_z,
    s_yout, r_yout, s_xout, r_xout, r_tail, s_back, r_back, s_d, r_d,
):
    count = logs_ref.shape[1] // BLOCK
    scale = DK ** (-0.5)
    half = HEAD_COUNT // CORES
    wx = DK // nx
    wy = wx // ny
    d_core, d_mate = decay_rows.at[0], decay_rows.at[1]
    d_x, d_y = decay_rows.at[pl.ds(2, nx)], decay_rows.at[pl.ds(2 + nx, ny)]
    d_z = decay_rows.at[pl.ds(2 + nx + ny, nz)]
    early = max(1, half - 2)
    chunks = [(d, k) for k in range(early) for d in range(2)]
    chunks += [(d, k) for d in (1, 0) for k in range(early, half)]
    grp, mem = lax.axis_index("grp"), lax.axis_index("mem")
    z, y = grp // ny, lax.rem(grp, ny)
    x, core = mem // CORES, lax.rem(mem, CORES)
    mate = (grp, x * CORES + 1 - core)

    def x_id(to):
        return (grp, to * CORES + core)

    def y_id(to):
        return (z * ny + to, mem)

    def z_id(to):
        return (to * ny + y, mem)

    xs = [lax.rem(x + off, nx) for off in range(1, nx)]
    ys = [lax.rem(y + off, ny) for off in range(1, ny)]
    zs = [lax.rem(z + off, nz) for off in range(1, nz)]
    barrier = pltpu.get_barrier_semaphore()

    def tell(sem, device):
        pl.semaphore_signal(sem, inc=1, device_id=device, device_id_type=MESH)

    for device in [(grp, o * CORES) for o in xs] + [(z * ny + o, x * CORES) for o in ys]:
        tell(barrier, device)
    pl.when(core == 1)(lambda: tell(barrier, mate))
    for o in zs:
        tell(barrier, (o * ny + y, x * CORES + 1))

    def hear(hearer, signals):
        @pl.when(core == hearer)
        def _():
            pl.semaphore_wait(barrier, signals)
            tell(s_meet, mate)

    def learn(hearer):
        @pl.when(core != hearer)
        def _():
            pl.semaphore_wait(s_meet, 1)

    def copy(src, dst, send, recv, device):
        return pltpu.make_async_remote_copy(
            src_ref=src, dst_ref=dst, send_sem=send, recv_sem=recv,
            device_id=device, device_id_type=MESH,
        )

    def go(*args):
        copy(*args).start()

    def landed(ref, sem):
        copy(ref, ref, s_back, sem, mate).wait_recv()

    def left(ref, sem):
        copy(ref, ref, sem, r_back.at[0], mate).wait_send()

    def members(d, size):
        return range(size) if d == 0 else range(size - 1, -1, -1)

    mine, theirs = core * half, (1 - core) * half

    def rows_of(c, size):
        return pl.ds(pl.multiple_of(c * size, size), size)

    def cols_of(head, size):
        return pl.ds(pl.multiple_of(head * size, size), size)

    def tokens_of(b):
        return pl.ds(b * BLOCK, BLOCK)

    load_logs = pltpu.make_async_copy(logs_hbm, logs_ref, s_logs)
    load_logs.start()

    def load(head, pair, slot):
        part = cols_of(head, DK)
        for i in (2 * pair, 2 * pair + 1):
            far = (k_hbm, v_hbm, q_hbm, g_hbm)[i]
            pltpu.make_async_copy(far.at[:, part], toks.at[i, :, part], s_in.at[slot]).start()

    load(theirs, 0, 0)

    def ready(slot, parts, heads):
        held = toks.at[pl.ds(0, parts), :, pl.ds(0, heads * DK)]
        pltpu.make_async_copy(held, held, s_in.at[slot]).wait()

    def tok(i, head, b):
        return toks[i, tokens_of(b), cols_of(head, DK)]

    square = (BLOCK, BLOCK)
    lower = lax.broadcasted_iota(jnp.int32, square, 0) >= lax.broadcasted_iota(jnp.int32, square, 1)
    ones = jnp.where(lower, 1.0, 0.0)
    load_logs.wait()
    load(mine, 0, 2)
    load(theirs, 1, 1)
    load(mine, 1, 1)
    carried = None
    for b in range(count):
        row = lax.dot_general(
            logs_ref[:, b * BLOCK:(b + 1) * BLOCK], ones, (((1,), (1,)), ((), ())),
            precision=lax.Precision.HIGHEST, preferred_element_type=F32,
        )
        for h in range(HEAD_COUNT):
            cum[b, h] = row[h:h + 1, :]
        whole = jnp.exp(row[:, BLOCK - 1:BLOCK])
        carried = whole if carried is None else carried * whole
    carried = jnp.broadcast_to(carried, (HEAD_COUNT, DV))
    for h in range(HEAD_COUNT):
        d_core[h] = carried[h:h + 1, :]
    def factors(head, b):
        row = cum[b, head]
        flat, cols = spread_rows(row)
        end = row[:, BLOCK - 1:BLOCK]
        return flat, cols, end

    def forward_total(head):
        forward = None
        for b in range(count):
            _, cols, end = factors(head, b)
            kd = tok(KEYS, head, b).astype(F32) * wide(jnp.exp(end - cols), DK)
            whole = jnp.broadcast_to(jnp.exp(end), (1, DV))
            part = dot(kd.astype(BF16), tok(VALUES, head, b), 0, 0)
            if b > 0:
                local[0, b - 1, head] = forward
            forward = part if forward is None else whole * forward + part
        total_buf[0, head] = forward

    def reverse_total(head):
        back = None
        for b in reversed(range(count)):
            _, cols, end = factors(head, b)
            qd = tok(QUERIES, head, b).astype(F32) * wide(jnp.exp(cols), DK)
            whole = jnp.broadcast_to(jnp.exp(end), (1, DV))
            part = dot(qd.astype(BF16), tok(GRADS, head, b), 0, 0)
            if b < count - 1:
                local[1, b, head] = back
            back = part if back is None else whole * back + part
        total_buf[1, head] = back

    def intra(head):
        for b in range(count):
            flat, cols, _ = factors(head, b)
            decay = jnp.where(lower, jnp.exp(jnp.where(lower, cols - flat, 0.0)), 0.0)
            q, k = tok(QUERIES, head, b), tok(KEYS, head, b)
            v, g = tok(VALUES, head, b), tok(GRADS, head, b)
            wg = (dot(g, v, 1, 1) * decay).astype(BF16)
            wv = (dot(q, k, 1, 1) * decay).astype(BF16)
            inner[0, head, tokens_of(b), :] = dot(wg, k, 1, 0)
            inner[1, head, tokens_of(b), :] = dot(wg, q, 0, 0)
            inner[2, head, tokens_of(b), :] = dot(wv, g, 0, 0)

    def outer(d, head, arrive=None):
        spreads = []
        for b in members(d, count):
            _, cols, end = factors(head, b)
            spreads.append((jnp.exp(cols if d == 0 else end - cols), jnp.exp(end)))
        if arrive is not None:
            arrive()
        coming = from_buf[d, head]
        weight = None
        for step, b in enumerate(members(d, count)):
            reach, last = spreads[step]
            if step == 0:
                low = coming.astype(BF16)
            else:
                low = (local[d, b - 1 if d == 0 else b, head] + weight * coming).astype(BF16)
            whole = jnp.broadcast_to(last, (1, DV))
            weight = whole if weight is None else weight * whole
            if d == 0:
                far = wide(reach, DK) * dot(tok(GRADS, head, b), low, 1, 1)
                near = inner[0, head, tokens_of(b), :]
                gq_ref[tokens_of(b), cols_of(head, DK)] = (scale * (near + far)).astype(BF16)
            else:
                tail = wide(reach, DK)
                near = inner[1, head, tokens_of(b), :]
                far = tail * dot(tok(VALUES, head, b), low, 1, 1)
                gk_ref[tokens_of(b), cols_of(head, DK)] = (scale * (near + far)).astype(BF16)
                near = inner[2, head, tokens_of(b), :]
                far = tail * dot(tok(KEYS, head, b), low, 1, 0)
                gv_ref[tokens_of(b), cols_of(head, DV)] = (scale * (near + far)).astype(BF16)

    first = core == 0

    def send_core(n, d, j):
        if n:
            go(total_buf.at[d, theirs + j], peer_buf.at[d, j], s_core, r_core.at[n // 2], mate)
        else:
            for i, o in enumerate(xs + [x]):
                part = rows_of(o, wx)
                go(total_buf.at[d, theirs + j, part, :], peer_buf.at[d, j, part, :],
                   s_core, r_first.at[i], mate)

    def join_cores(n, d, j):
        if n == 1:
            landed(peer_buf.at[d, j], r_core.at[0])
        elif n and n % 2 == 0:
            landed(peer_buf.at[0, pl.ds(0, 2)], r_core.at[n // 2])
        own_d, peer_d = d_core[mine + j], d_mate[mine + j]
        one = jnp.ones_like(own_d)
        if d == 0:
            w_own, w_peer = jnp.where(first, peer_d, one), jnp.where(first, one, own_d)
        else:
            w_own, w_peer = jnp.where(first, one, peer_d), jnp.where(first, own_d, one)

        def joined(o):
            part = rows_of(o, wx)
            return w_own * total_buf[d, mine + j, part, :] + w_peer * peer_buf[d, j, part, :]

        for i, o in enumerate(xs):
            if n == 0:
                landed(peer_buf.at[d, j, rows_of(o, wx), :], r_first.at[i])
            chip_buf[d, j, rows_of(o, wx), :] = joined(o)
            go(chip_buf.at[d, j, rows_of(o, wx), :], x_in.at[x, d, j], s_x, r_x.at[n], x_id(o))
        if n == 0:
            landed(peer_buf.at[d, j, rows_of(x, wx), :], r_first.at[nx - 1])
        x_in[x, d, j] = joined(x)

    def fold(d, j, parts, decays, size):
        running = None
        for c in members(d, size):
            part = parts[c, d, j]
            running = part if running is None else decays[c, mine + j] * running + part
        return running

    def up_x(n, d, j):
        if n == 0:
            landed(d_x.at[pl.ds(0, nx - 1)], r_d.at[1])
            product = d_x[0]
            for c in range(1, nx):
                product = product * d_x[c]
            d_y[y] = product
            for o in ys:
                go(d_y.at[y], d_y.at[y], s_d, r_d.at[2], y_id(o))
        landed(x_in.at[pl.ds(0, nx - 1), d, j], r_x.at[n])
        row_tot[d, j] = fold(d, j, x_in, d_x, nx)
        for o in ys:
            go(row_tot.at[d, j, rows_of(o, wy), :], y_in.at[y, d, j], s_y, r_y.at[n], y_id(o))
        y_in[y, d, j] = row_tot[d, j, rows_of(y, wy), :]

    def up_y(n, d, j):
        if n == 0:
            if ny > 1:
                landed(d_y.at[pl.ds(0, ny - 1)], r_d.at[2])
            product = d_y[0]
            for c in range(1, ny):
                product = product * d_y[c]
            d_z[z] = product
            if nz > 1:
                hear(1, CORES * (nz - 1))
                learn(1)
            for t in zs:
                go(d_z.at[z], d_z.at[z], s_d, r_d.at[3], z_id(t))
        if ny > 1:
            landed(y_in.at[pl.ds(0, ny - 1), d, j], r_y.at[n])
        plane_tot[d, j] = fold(d, j, y_in, d_y, ny)
        send_z(n, d, j, 0, plane_tot.at[d, j])

    levels = (nz - 1).bit_length()
    shared = max(0, levels - 2)

    def place(d):
        return z if d == 0 else nz - 1 - z

    def z_sends(d, level):
        size, p = 1 << level, place(d)
        last = lax.rem(p, 2 * size) == size - 1
        return [(i + 1, jnp.logical_and(last, p + i + 1 < nz)) for i in range(size)]

    def z_hears(d, level):
        return lax.rem(place(d), 2 << level) >= 1 << level

    def send_z(n, d, j, level, src):
        if level < levels:
            for hop, needed in z_sends(d, level):
                to = lax.rem(z + hop, nz) if d == 0 else lax.rem(z - hop + nz, nz)
                c = copy(src, z_in.at[2 * level + d, j], s_z, r_z.at[min(level, shared), n], z_id(to))
                pl.when(needed)(c.start)

    def z_weight(d, level):
        size = 1 << level
        start = place(d) // size * size
        weight = jnp.ones_like(d_core[...])
        for i in range(size - 1):
            q = lax.rem(start + i, nz)
            passed = d_z[q if d == 0 else nz - 1 - q]
            weight = jnp.where(start + i < place(d), weight * passed, weight)
        return weight

    def spread(d, j, held, parts, decays, size, out):
        last = members(d, size)[-1]
        for c in members(d, size):
            out[c, d, j] = held
            if c != last:
                held = decays[c, mine + j] * held + parts[c, d, j]

    def over_z(level, n, d, j):
        if n == 0 and level == 0:
            landed(d_z.at[pl.ds(0, nz - 1)], r_d.at[3])
            for side in range(2):
                for upper in range(levels):
                    weights[upper, side] = z_weight(side, upper)
        if level == 0:
            z_carry[d, j] = jnp.zeros((wy, DV), F32)

        def hear_z():
            came = z_in[2 * level + d, j]
            if level:
                came = weights[level, d, mine + j] * came + z_carry[d, j]
            z_carry[d, j] = came

        hears = z_hears(d, level)
        if level == levels - 1 and level:
            both = jnp.logical_and(hears, z_hears(d, level - 1))

            @pl.when(both)
            def _():
                landed(z_in.at[pl.ds(0, 2), j], r_z.at[shared, n])
                early = z_in[2 * (level - 1) + d, j]
                if level > 1:
                    early = weights[level - 1, d, mine + j] * early + z_carry[d, j]
                z_carry[d, j] = early
                hear_z()

            @pl.when(jnp.logical_and(hears, jnp.logical_not(both)))
            def _():
                landed(z_in.at[2 * level + d, j], r_z.at[shared, n])
                hear_z()
        else:
            alone = hears
            if level == levels - 2:
                alone = jnp.logical_and(hears, jnp.logical_not(z_hears(d, level + 1)))

            @pl.when(alone)
            def _():
                landed(z_in.at[2 * level + d, j], r_z.at[level, n])
                hear_z()

        if level + 1 < levels:
            @pl.when(z_sends(d, level + 1)[0][1])
            def _():
                z_out[level, d, j] = d_z[z, mine + j] * z_carry[d, j] + plane_tot[d, j]

            send_z(n, d, j, level + 1, z_out.at[level, d, j])

    def down_z(n, d, j):
        if levels:
            over_z(levels - 1, n, d, j)
        else:
            z_carry[d, j] = jnp.zeros((wy, DV), F32)
        spread(d, j, z_carry[d, j], y_in, d_y, ny, y_out)
        send_y(n, d, j)

    def send_y(n, d, j):
        for o in ys:
            go(y_out.at[o, d, j], row_carry.at[d, j, rows_of(y, wy), :], s_yout, r_yout.at[n], y_id(o))
        row_carry[d, j, rows_of(y, wy), :] = y_out[y, d, j]

    def starts(d, at):
        row = jnp.logical_and(z == (0 if d == 0 else nz - 1), y == (0 if d == 0 else ny - 1))
        return jnp.logical_and(row, at == (0 if d == 0 else nx - 1))

    final = len(chunks) - 1

    def send_x(n, d, j, part=None, ready=True):
        size = wx if part is None else wx // 2
        start = 0 if part is None else part * size
        sem = r_tail if part == 1 else r_xout.at[n]
        for o in xs:
            c = copy(
                x_out.at[o, d, j, pl.ds(start, size), :],
                carry.at[d, j, pl.ds(pl.multiple_of(x * wx + start, size), size), :],
                s_xout.at[d], sem, x_id(o),
            )
            pl.when(jnp.logical_and(jnp.logical_not(starts(d, o)), ready))(c.start)

    def down_y(n, d, j):
        if ny > 1:
            landed(row_carry.at[d, j, pl.ds(0, (ny - 1) * wy), :], r_yout.at[n])
        spread(d, j, row_carry[d, j], x_in, d_x, nx, x_out)
        if n == final:
            for part in range(2):
                send_x(n, d, j, part, core == 0)
        else:
            send_x(n, d, j)
        carry[d, j, rows_of(x, wx), :] = x_out[x, d, j]
        if n == final:
            send_back(n, d, j, rows_of(x, wx))

    def down_x(n, d, j):
        starting = starts(d, x)

        def come(ref, sem):
            @pl.when(starting)
            def _():
                for o in xs:
                    carry[d, j, rows_of(o, wx), :] = jnp.zeros((wx, DV), F32)

            pl.when(jnp.logical_not(starting))(lambda: landed(ref, sem))

        if n == final:
            size = wx // 2
            for part in range(2):
                come(carry.at[d, j, pl.ds(0, (nx - 1) * size), :], r_tail if part else r_xout.at[n])
                for o in xs:
                    start = pl.multiple_of(o * wx + part * size, size)
                    send_back(n, d, j, pl.ds(start, size))
        else:
            come(carry.at[d, j, pl.ds(0, (nx - 1) * wx), :], r_xout.at[n])
            if n == final - 1:
                send_x(final, *chunks[final], 0, core != 0)
            send_back(n, d, j, pl.ds(0, DK))
        outer(d, mine + j)

    def send_back(n, d, j, part):
        near = first if d == 0 else jnp.logical_not(first)

        @pl.when(near)
        def _():
            got = carry[d, j, part, :]
            back_buf[d, j, part, :] = d_core[mine + j] * got + total_buf[d, mine + j, part, :]
            from_buf[d, mine + j, part, :] = got

        @pl.when(jnp.logical_not(near))
        def _():
            got = carry[d, j, part, :]
            back_buf[d, j, part, :] = got
            from_buf[d, mine + j, part, :] = d_mate[mine + j] * got + peer_buf[d, j, part, :]

        go(back_buf.at[d, j, part, :], from_buf.at[d, mine + j, part, :], s_back, r_back.at[n], mate)

    def finish(n, d, j):
        outer(d, theirs + j, lambda: landed(from_buf.at[d, theirs + j], r_back.at[n]))

    def load_more(k):
        for head in (theirs + k, mine + k):
            load(head, 0, k + 2)
            load(head, 1, k + 2)

    def greet_mate():
        go(d_core, d_mate, s_d, r_d.at[0], mate)
        send_core(0, *chunks[0])

    totals = (forward_total, reverse_total)
    ready(0, 2, 1)
    forward_total(theirs)
    hear(0, 1 + CORES * (nx + ny - 2))
    pl.when(core == 0)(greet_mate)
    ready(2, 2, 1)
    forward_total(mine)
    learn(0)
    pl.when(core != 0)(greet_mate)
    load_more(1)
    ready(1, 4, 1)
    reverse_total(theirs)
    send_core(1, *chunks[1])
    landed(d_mate, r_d.at[0])
    d_x[x] = d_core[...] * d_mate[...]
    for o in xs:
        go(d_x.at[x], d_x.at[x], s_d, r_d.at[1], x_id(o))
    join_cores(0, *chunks[0])
    for k in range(2, half):
        load_more(k)
    reverse_total(mine)
    join_cores(1, *chunks[1])
    late, held = [], {0}
    for turn in (range(n, n + 2) for n in range(2, len(chunks), 2)):
        for n in turn:
            d, k = chunks[n]
            if k not in held:
                ready(k + 2, 4, CORES)
                held.add(k)
            totals[d](theirs + k)
            send_core(n, d, k)
            for m in late:
                join_cores(m, *chunks[m])
            late = []
        for n in turn:
            totals[chunks[n][0]](mine + chunks[n][1])
        join_cores(turn[0], *chunks[turn[0]])
        late = turn[1:]
    for m in late:
        join_cores(m, *chunks[m])

    def inside(n, d, j):
        for h in range(n, HEAD_COUNT, len(chunks)):
            intra(h)

    climb = [(2 + level, functools.partial(over_z, level)) for level in range(levels - 1)]
    top = 2 + len(climb)
    back = len(chunks)
    stages = [(0, up_x), (0, inside), (top + 3, down_y), (back + 2, finish), (back, down_x)]
    stages += [(1, up_y)] + climb + [(top + 1, down_z)]
    for slot in range(2 * len(chunks) + 1):
        for lag, stage in stages:
            n = slot - lag
            if stage is finish and n >= final - 1:
                n = final
            if 0 <= n < len(chunks):
                stage(n, *chunks[n])
            if stage is finish and n == final - 2:
                send_x(final, *chunks[final], 1, core != 0)
                finish(final - 1, *chunks[final - 1])

    left(peer_buf, s_core)
    left(x_in.at[pl.ds(0, nx - 1)], s_x)
    withheld = [
        sum(jnp.where(starts(d, o), 1, 0) for o in xs) for d in range(2)
    ]
    for d in range(2):
        for amount in (nx - 2, nx - 1):
            if amount:
                pl.when(withheld[d] == nx - 1 - amount)(
                    functools.partial(left, x_out.at[pl.ds(0, amount), d], s_xout.at[d])
                )
    left(back_buf, s_back)
    left(decay_rows.at[pl.ds(0, nx + ny + nz - 2)], s_d)
    if ny > 1:
        left(y_in.at[pl.ds(0, ny - 1)], s_y)
        left(y_out.at[pl.ds(0, ny - 1)], s_yout)
    if nz > 1:
        sends = sum(
            jnp.where(needed, 1, 0)
            for level in range(levels) for d in range(2) for _, needed in z_sends(d, level)
        )
        for amount in range(1, nz):
            pl.when(sends == amount)(functools.partial(left, z_in.at[pl.ds(0, amount)], s_z))


def write_kernel(gq_ref, gk_ref, gv_ref, gq_hbm, gk_hbm, gv_hbm, sems):
    copies = [
        pltpu.make_async_copy(near, far, sems.at[i])
        for i, (near, far) in enumerate(((gq_ref, gq_hbm), (gk_ref, gk_hbm), (gv_ref, gv_hbm)))
    ]
    for c in copies:
        c.start()
    for c in copies:
        c.wait()


def body(nx, ny, nz, queries, keys, values, grad_out, log_decay):
    tokens = queries.shape[0]
    count = tokens // BLOCK
    half = HEAD_COUNT // CORES
    wx = DK // nx
    wy = wx // ny
    levels = (nz - 1).bit_length()
    n = 2 * half
    vm = pl.BlockSpec(memory_space=pltpu.VMEM)
    hbm = pl.BlockSpec(memory_space=pltpu.HBM)
    dma = pltpu.SemaphoreType.DMA

    def states(*lead):
        return pltpu.VMEM(lead + (DV,), F32)

    def decays(*lead):
        return pltpu.VMEM(lead + (HEAD_COUNT, 1, DV), F32)

    out = jax.ShapeDtypeStruct((tokens, HEAD_COUNT * DK), BF16)
    near = pltpu.VMEM(out.shape, out.dtype)
    grads = pl.pallas_call(
        functools.partial(retention_kernel, nx, ny, nz),
        out_shape=(near, near, near),
        in_specs=[hbm] * 5,
        out_specs=(vm, vm, vm),
        scratch_shapes=[
            pltpu.VMEM((HEAD_COUNT, tokens), F32),
            pltpu.VMEM((4, tokens, HEAD_COUNT * DK), BF16),
            pltpu.VMEM((count, HEAD_COUNT, 1, BLOCK), F32),
            states(2, max(1, count - 1), HEAD_COUNT, DK),
            states(3, HEAD_COUNT, tokens),
            states(2, HEAD_COUNT, DK), states(2, HEAD_COUNT, DK),
            states(2, half, DK), states(2, half, DK),
            states(2, half, DK), states(nx, 2, half, wx), states(2, half, wx),
            states(ny, 2, half, wy), states(2, half, wy),
            states(max(2 * levels, nz), half, wy), states(max(1, levels - 1), 2, half, wy), states(2, half, wy),
            states(ny, 2, half, wy), states(2, half, wx),
            states(nx, 2, half, wx), states(2, half, DK),
            decays(2 + nx + ny + nz), decays(max(1, levels), 2), pltpu.SemaphoreType.REGULAR, dma, dma((half + 2,)),
            dma, dma((half,)), dma((nx,)), dma, dma((n,)), dma, dma((n,)), dma, dma((max(1, levels - 1), n)),
            dma, dma((n,)), dma((2,)), dma((n,)), dma, dma, dma((n,)), dma, dma((4,)),
        ],
        compiler_params=pltpu.CompilerParams(collective_id=0, has_side_effects=True, vmem_limit_bytes=52 << 20),
        name="retention",
    )(pltpu.with_memory_space_constraint(log_decay, pltpu.HBM), queries, keys, values, grad_out)
    return pl.pallas_call(
        write_kernel,
        out_shape=(out, out, out),
        in_specs=[vm] * 3,
        out_specs=(hbm, hbm, hbm),
        scratch_shapes=[dma((3,))],
        name="write",
    )(*(pltpu.with_memory_space_constraint(g, pltpu.VMEM) for g in grads))


def solution(mesh):
    nx = mesh.shape["mem"] // CORES
    ny = nx if mesh.shape["grp"] % nx == 0 else 1
    nz = mesh.shape["grp"] // ny
    tokens = P(("grp", "mem"), None)
    return jax.shard_map(
        functools.partial(body, nx, ny, nz),
        mesh=mesh,
        in_specs=(tokens, tokens, tokens, tokens, P(None, ("grp", "mem"))),
        out_specs=(tokens, tokens, tokens),
        check_vma=False,
    )
```
